256 devices in a mesh: batch: 128 (over z, y, x_lo, core), rep: 2 (over x_hi).
Axes of the slice: x: 4 (x_hi: 2, x_lo: 2; x = x_hi * 2 + x_lo), y: 4, z: 8, core: 2. Of those that a mesh axis runs over, the one named last changes fastest.
Arguments:
- queries: bfloat16 [16384, 512], P('batch', 'rep'), may hold values from -8 to 8
- passages: bfloat16 [16384, 512], P('batch', 'rep'), may hold values from -8 to 8
- positives: int32 [16384], replicated, may hold values from 0 to 16383, each once
Outputs:
- grad_queries: float32 [16384, 512], P('batch', 'rep')
- grad_passages: float32 [16384, 512], P('batch', 'rep')
The draws below stay inside these ranges and needn't reach their ends.
Inputs may be any that keep to these rules, and one draw needn't show every extreme that they name: `positives`: each passage is the positive of exactly one query.
All inputs are finite; a program needn't handle non-finite values.
Results may differ from the reference program's by a relative error of at most 0.0013.
Values may be sent and summed in bfloat16 or wider, within the bound.
A program may use at most 128 MiB of HBM per device.

```python
import math
import jax
import jax.numpy as jnp
from jax import lax

D = 512
TOTAL = 16384


def embedding_draw(key, member):
    member_key = jax.random.fold_in(key, member + 11)
    scale_key, entry_key = jax.random.split(member_key, 2)
    row_scale = jnp.exp(jax.random.uniform(scale_key, (TOTAL, 1), jnp.float32, math.log(0.3), math.log(3.0)))
    entries = jax.random.normal(entry_key, (TOTAL, D), jnp.float32)
    values = jnp.clip(row_scale * entries, -8.0, 8.0)
    return values.astype(jnp.bfloat16)


def draw_queries(key, part):
    return embedding_draw(key, 0)


def draw_passages(key, part):
    return embedding_draw(key, 1)


def setup_inputs(seed: int = 0) -> dict:
    key_list = jax.random.split(jax.random.key(seed), 4)
    return {
        "queries": draw_queries(jax.random.fold_in(key_list[3], 71), 0),
        "passages": draw_passages(jax.random.fold_in(key_list[3], 71), 0),
        "positives": jax.random.permutation(key_list[2], TOTAL).astype(jnp.int32),
    }


def block_scores(query_block, passages, logit_scale):
    return jnp.dot(query_block, passages.T, preferred_element_type=jnp.float32) * logit_scale

def reference(queries, passages, positives):
    logit_scale = 1.0 / math.sqrt(D)
    block_rows = math.gcd(TOTAL, 512)
    block_count = TOTAL // block_rows
    query_blocks = queries.reshape(block_count, block_rows, D)
    positive_blocks = positives.reshape(block_count, block_rows)

    def first_sweep(running, query_block):
        column_high, column_total = running
        scores = block_scores(query_block, passages, logit_scale)
        row_high = lax.optimization_barrier(jnp.max(scores, axis=1))
        row_norm = row_high + jnp.log(lax.optimization_barrier(jnp.sum(jnp.exp(scores - row_high[:, None]), axis=1)))
        new_high = jnp.maximum(column_high, lax.optimization_barrier(jnp.max(scores, axis=0)))
        column_total = column_total * jnp.exp(column_high - new_high) + lax.optimization_barrier(jnp.sum(jnp.exp(scores - new_high[None, :]), axis=0))
        return ((new_high, column_total), row_norm)
    starting = (jnp.full((TOTAL,), -1e+30, jnp.float32), jnp.zeros((TOTAL,), jnp.float32))
    (column_high, column_total), row_norms = lax.scan(first_sweep, starting, query_blocks)
    column_norms = column_high + jnp.log(column_total)
    passage_ids = jnp.arange(TOTAL, dtype=jnp.int32)

    def second_sweep(grad_passages, inputs):
        query_block, row_block, positive_block = inputs
        scores = block_scores(query_block, passages, logit_scale)
        matches = (positive_block[:, None] == passage_ids[None, :]).astype(jnp.float32)
        weights = jnp.exp(scores - row_block[:, None]) + jnp.exp(scores - column_norms[None, :]) - 2.0 * matches
        weights = weights.astype(jnp.bfloat16)
        grad_block = jnp.dot(weights, passages, preferred_element_type=jnp.float32) * logit_scale
        grad_passages = grad_passages + jnp.dot(weights.T, query_block, preferred_element_type=jnp.float32) * logit_scale
        return (grad_passages, grad_block)
    grad_passages, grad_blocks = lax.scan(second_sweep, jnp.zeros((TOTAL, D), jnp.float32), (query_blocks, row_norms, positive_blocks))
    return (grad_blocks.reshape(TOTAL, D), grad_passages)
```

```python
import math

import jax
import jax.numpy as jnp
from jax import lax
from jax.experimental import pallas as pl
from jax.experimental.pallas import tpu as pltpu
from jax.sharding import Mesh
from jax.sharding import PartitionSpec as P

AXES = ("z", "y", "xl", "c", "xh")
BATCH = ("z", "y", "xl", "c")
NX, NY, NZ = 4, 4, 8
MESH = pl.DeviceIdType.MESH
ROWS = 128
HALF = 64
WIDE = 256
TILE = 1024
STEP = 32000.0
LOG2E = 1.4426950408889634
LN2 = 0.6931471805599453


def encode(x):
    top = jnp.max(jnp.abs(x), axis=0, keepdims=True)
    power = jnp.clip(jnp.floor(jnp.log(top) * LOG2E) + 1.0, -120.0, 120.0)
    value = jnp.round(x * (STEP * jnp.exp2(-power)))
    power = jnp.broadcast_to(power, (16, x.shape[1]))
    return (
        value.astype(jnp.int32).astype(jnp.int16),
        power.astype(jnp.int32).astype(jnp.int16),
    )


def decode(value, power):
    unit = jnp.exp2(power.astype(jnp.int32).astype(jnp.float32)[:1]) * (1.0 / STEP)
    return value.astype(jnp.int32).astype(jnp.float32) * unit


def to_lanes(column):
    return jnp.broadcast_to(column, (128, 128)).T[:1]


def to_rows(line):
    return jnp.broadcast_to(line, (128, 128)).T


def join(stack):
    high = jnp.max(stack, axis=0)
    return high + jnp.log(jnp.sum(jnp.exp2(stack - high[None]), axis=0)) * LOG2E


def nt(a, b):
    return lax.dot_general(a, b, (((1,), (1,)), ((), ())), preferred_element_type=jnp.float32)


def tn(a, b):
    return lax.dot_general(a, b, (((0,), (0,)), ((), ())), preferred_element_type=jnp.float32)


def kernel(
    q_ref, p_ref, pos_ref, gq_ref, gp_ref,
    Q, PT, S, W, posc, tmp, cmax, csum, rstat, cstat, rown, cown, rfin,
    XQ, GQ, SQ, RQ, SP, RP,
    s_xq, r_xq, s_p, r_p, s_q, r_q, s_d, r_d, s_rs, r_rs, s_cs, r_cs,
    s_x, r_x, s_gp, r_gp, s_gq, r_gq,
):
    z, y, xl, c, xh = (lax.axis_index(a) for a in AXES)
    x = xh * 2 + xl
    factor = 1.0 / math.sqrt(2 * WIDE)

    def copy(src, dst, ssem, rsem, **where):
        return pltpu.make_async_remote_copy(
            src_ref=src, dst_ref=dst, send_sem=ssem, recv_sem=rsem,
            device_id=where, device_id_type=MESH,
        )

    def plane(k):
        tx, ty = lax.rem(x + k % 4, NX), lax.rem(y + k // 4, NY)
        return tx, ty, {"xh": tx // 2, "xl": lax.rem(tx, 2), "y": ty}

    def plane_from(k):
        fx, fy = lax.rem(x + (4 - k % 4) % 4, NX), lax.rem(y + (4 - k // 4) % 4, NY)
        return fx, fy

    def pillar(k):
        tz, tc = lax.rem(z + k // 2, NZ), lax.rem(c + k % 2, 2)
        return tz, tc, {"z": tz, "c": tc}

    def pillar_from(k):
        return lax.rem(z + (8 - k // 2) % 8, NZ), lax.rem(c + k % 2, 2)

    barrier = pltpu.get_barrier_semaphore()
    count = 0
    for k in range(1, 16):
        for where in (plane(k)[2], pillar(k)[2]):
            pl.semaphore_signal(barrier, inc=1, device_id=where, device_id_type=MESH)
            count += 1
    for k in range(NZ):
        where = {"xh": 1 - xh, "z": lax.rem(z + k, NZ)}
        if k:
            pl.semaphore_signal(barrier, inc=1, device_id=where, device_id_type=MESH)
            count += 1
    pl.semaphore_wait(barrier, count)

    slot_q = z * 2 + c
    slot_p = y * 2 + xl
    own_rows = pl.ds(pl.multiple_of(xh * HALF, HALF), HALF)
    other_rows = pl.ds(pl.multiple_of((1 - xh) * HALF, HALF), HALF)

    sends = []
    cp = copy(q_ref.at[other_rows], Q.at[xh, slot_q], s_xq, r_xq, xh=1 - xh)
    cp.start()
    sends.append(cp)
    for k in range(1, 8):
        for_a = copy(q_ref.at[own_rows], Q.at[xh, slot_q], s_q.at[0, k], r_q.at[0, k], z=lax.rem(z + k, NZ))
        for_a.start()
        sends.append(for_a)
    for k in range(1, 16):
        cp = copy(p_ref, PT.at[xh, slot_p], s_p.at[k], r_p.at[k], **plane(k)[2])
        cp.start()
        sends.append(cp)
    copy(q_ref.at[own_rows], Q.at[1 - xh, slot_q], s_xq, r_xq, xh=1 - xh).wait_recv()
    for k in range(1, 8):
        cp = copy(Q.at[1 - xh, slot_q], Q.at[1 - xh, slot_q], s_q.at[1, k], r_q.at[1, k], z=lax.rem(z + k, NZ))
        cp.start()
        sends.append(cp)
    Q[xh, slot_q] = q_ref[own_rows, :]
    PT[xh, slot_p] = p_ref[...]
    cp = copy(q_ref.at[own_rows], Q.at[xh, slot_q], s_d.at[0], r_d.at[0], c=1 - c)
    cp.start()
    sends.append(cp)
    cp = copy(Q.at[1 - xh, slot_q], Q.at[1 - xh, slot_q], s_d.at[8], r_d.at[8], c=1 - c)
    cp.start()
    sends.append(cp)

    for s in range(16):
        line = (s // 2) * 16 + y * 4 + xl * 2 + s % 2
        tmp[...] = to_rows(pos_ref[pl.ds(line, 1), :])
        posc[s * HALF : (s + 1) * HALF] = tmp[own_rows, :]

    for k in range(1, 8):
        fz = lax.rem(z + 8 - k, NZ)
        for h, part in ((0, xh), (1, 1 - xh)):
            copy(Q.at[part, slot_q], Q.at[part, fz * 2 + c], s_q.at[h, k], r_q.at[h, k], z=fz).wait_recv()
        cp = copy(Q.at[:, fz * 2 + c], Q.at[:, fz * 2 + c], s_d.at[k], r_d.at[k], c=1 - c)
        cp.start()
        sends.append(cp)
    for k in range(1, 16):
        fx, fy = plane_from(k)
        copy(p_ref, PT.at[fx // 2, fy * 2 + lax.rem(fx, 2)], s_p.at[k], r_p.at[k], c=1 - c).wait_recv()
    for k in range(0, 8):
        fz = lax.rem(z + 8 - k, NZ)
        if k == 0:
            copy(q_ref.at[own_rows], Q.at[xh, z * 2 + 1 - c], s_d.at[0], r_d.at[0], c=1 - c).wait_recv()
            copy(q_ref.at[own_rows], Q.at[1 - xh, z * 2 + 1 - c], s_d.at[8], r_d.at[8], c=1 - c).wait_recv()
        else:
            copy(Q.at[:, slot_q], Q.at[:, fz * 2 + 1 - c], s_d.at[k], r_d.at[k], c=1 - c).wait_recv()

    def score(i, carry):
        rows = pl.ds(pl.multiple_of(i * 128, 128), 128)
        part = [
            nt(Q[h, pl.ds(i * 2, 2)].reshape(128, WIDE), PT[h].reshape(TILE, WIDE))
            for h in range(2)
        ]
        s = (part[0] + part[1]) * (factor * LOG2E)
        S[rows] = s
        high = jnp.max(s, axis=1, keepdims=True)
        total = jnp.sum(jnp.exp2(s - high), axis=1, keepdims=True)
        rown[pl.ds(i, 1)] = to_lanes(high + jnp.log(total) * LOG2E)
        chigh = jnp.max(s, axis=0, keepdims=True)
        cmax[pl.ds(i, 1)] = chigh
        csum[pl.ds(i, 1)] = jnp.sum(jnp.exp2(s - chigh), axis=0, keepdims=True)
        return carry

    lax.fori_loop(0, 8, score, 0)
    chigh = jnp.max(cmax[...], axis=0, keepdims=True)
    ctotal = jnp.sum(csum[...] * jnp.exp2(cmax[...] - chigh), axis=0, keepdims=True)
    cnorm = chigh + jnp.log(ctotal) * LOG2E
    for b in range(8):
        cown[b : b + 1] = cnorm[:, b * 128 : (b + 1) * 128]
    rstat[0] = rown[...]
    cstat[0] = cown[...]
    for k in range(1, 16):
        cp = copy(rown, rstat.at[k], s_rs.at[k], r_rs.at[k], **pillar(k)[2])
        cp.start()
        sends.append(cp)
        cp = copy(cown, cstat.at[k], s_cs.at[k], r_cs.at[k], **plane(k)[2])
        cp.start()
        sends.append(cp)
    for k in range(1, 16):
        copy(rown, rstat.at[k], s_rs.at[k], r_rs.at[k], **pillar(k)[2]).wait_recv()
        copy(cown, cstat.at[k], s_cs.at[k], r_cs.at[k], **plane(k)[2]).wait_recv()
    rown2 = join(rstat[...])
    cown2 = join(cstat[...])
    cmax[0:1] = jnp.concatenate([cown2[b : b + 1] for b in range(8)], axis=1)
    rfin[...] = rown2

    def weigh(i, carry):
        rows = pl.ds(pl.multiple_of(i * 128, 128), 128)
        rnorm = to_rows(rfin[pl.ds(i, 1), :])
        for b in range(8):
            cols = slice(b * 128, (b + 1) * 128)
            s = S[rows, cols]
            first = ((z * 4 + b // 2) * 2 + b % 2) * 2 + c
            ids = first * ROWS + lax.broadcasted_iota(jnp.int32, (128, 128), 1)
            match = jnp.where(posc[rows, :] == ids, 2.0, 0.0)
            w = jnp.exp2(s - rnorm) + jnp.exp2(s - cmax[0:1, cols]) - match
            W[rows, cols] = w.astype(jnp.bfloat16)
        return carry

    lax.fori_loop(0, 8, weigh, 0)

    for k in range(8):
        tz = lax.rem(z + k, NZ)
        rows = pl.ds(pl.multiple_of(tz * 128, 128), 128)
        for h in range(2):
            part = jnp.dot(W[rows, :], PT[h].reshape(TILE, WIDE), preferred_element_type=jnp.float32)
            tmp2 = part.reshape(2, HALF, WIDE)
            GQ[k, 0, h] = tmp2[0]
            GQ[k, 1, h] = tmp2[1]
        cp = copy(GQ.at[k, 1 - c], XQ.at[k], s_x.at[k], r_x.at[k], c=1 - c)
        cp.start()
        sends.append(cp)

    def send_queries(k):
        copy(GQ.at[k, 1 - c], XQ.at[k], s_x.at[k], r_x.at[k], c=1 - c).wait_recv()
        tz = lax.rem(z + k, NZ)
        for d in range(2):
            h = lax.rem(xh + d, 2)
            value, power = encode(GQ[k, c, h] + XQ[k, h])
            if k == 0 and d == 0:
                RQ[0, 0, 0:HALF] = value
                RQ[0, 0, HALF:] = power
                continue
            SQ[k, d, 0:HALF] = value
            SQ[k, d, HALF:] = power
            cp = copy(SQ.at[k, d], RQ.at[k, d], s_gq.at[k, d], r_gq.at[k, d], z=tz, xh=h)
            cp.start()
            sends.append(cp)

    order = [k for k in range(1, 16)] + [0]
    for n, k in enumerate(order):
        tx, ty, where = plane(k)
        cols = pl.ds(pl.multiple_of((ty * 2 + lax.rem(tx, 2)) * 128, 128), 128)
        value, power = encode(tn(W[:, cols], Q[tx // 2].reshape(TILE, WIDE)))
        if k == 0:
            RP[0, 0:ROWS] = value
            RP[0, ROWS:] = power
        else:
            SP[k, 0:ROWS] = value
            SP[k, ROWS:] = power
            cp = copy(SP.at[k], RP.at[k], s_gp.at[k], r_gp.at[k], **where)
            cp.start()
            sends.append(cp)
        if n % 2 == 1:
            send_queries((n // 2 + 1) % 8)

    total = jnp.zeros((ROWS, WIDE), jnp.float32)
    for k in range(16):
        if k:
            copy(SP.at[k], RP.at[k], s_gp.at[k], r_gp.at[k], **plane(k)[2]).wait_recv()
        total = total + decode(RP[k, 0:ROWS], RP[k, ROWS:])
    gp_ref[...] = total * factor
    for d in range(2):
        total = jnp.zeros((HALF, WIDE), jnp.float32)
        for k in range(8):
            if k or d:
                copy(SQ.at[k, d], RQ.at[k, d], s_gq.at[k, d], r_gq.at[k, d], z=lax.rem(z + k, NZ)).wait_recv()
            total = total + decode(RQ[k, d, 0:HALF], RQ[k, d, HALF:])
        gq_ref[(own_rows, other_rows)[d], :] = total * factor
    for cp in sends:
        cp.wait_send()


def local(queries, passages, positives):
    dma = pltpu.SemaphoreType.DMA
    vmem = pl.BlockSpec(memory_space=pltpu.VMEM)
    out = jax.ShapeDtypeStruct((ROWS, WIDE), jnp.float32)
    bf16, f32, i16 = jnp.bfloat16, jnp.float32, jnp.int16
    return pl.pallas_call(
        kernel,
        out_shape=(out, out),
        in_specs=[vmem] * 3,
        out_specs=(vmem, vmem),
        scratch_shapes=[
            pltpu.VMEM((2, 16, HALF, WIDE), bf16),
            pltpu.VMEM((2, 8, ROWS, WIDE), bf16),
            pltpu.VMEM((TILE, TILE), f32),
            pltpu.VMEM((TILE, TILE), bf16),
            pltpu.VMEM((TILE, 128), jnp.int32),
            pltpu.VMEM((128, 128), jnp.int32),
            pltpu.VMEM((8, TILE), f32),
            pltpu.VMEM((8, TILE), f32),
            pltpu.VMEM((16, 8, 128), f32),
            pltpu.VMEM((16, 8, 128), f32),
            pltpu.VMEM((8, 128), f32),
            pltpu.VMEM((8, 128), f32),
            pltpu.VMEM((8, 128), f32),
            pltpu.VMEM((8, 2, HALF, WIDE), f32),
            pltpu.VMEM((8, 2, 2, HALF, WIDE), f32),
            pltpu.VMEM((8, 2, HALF + 16, WIDE), i16),
            pltpu.VMEM((8, 2, HALF + 16, WIDE), i16),
            pltpu.VMEM((16, ROWS + 16, WIDE), i16),
            pltpu.VMEM((16, ROWS + 16, WIDE), i16),
            dma, dma,
            dma((16,)), dma((16,)),
            dma((2, 8)), dma((2, 8)),
            dma((9,)), dma((9,)),
            dma((16,)), dma((16,)),
            dma((16,)), dma((16,)),
            dma((8,)), dma((8,)),
            dma((16,)), dma((16,)),
            dma((8, 2)), dma((8, 2)),
        ],
        compiler_params=pltpu.CompilerParams(
            collective_id=0, has_side_effects=True, vmem_limit_bytes=60 * 1024 * 1024
        ),
    )(queries, passages, positives.reshape(128, 128))


def solution(mesh):
    split = Mesh(
        mesh.devices.reshape(NZ, NY, 2, 2, mesh.shape["rep"]),
        AXES,
    )
    return jax.shard_map(
        local,
        mesh=split,
        in_specs=(P(BATCH, "xh"), P(BATCH, "xh"), P()),
        out_specs=(P(BATCH, "xh"), P(BATCH, "xh")),
        check_vma=False,
    )
```

```python
import math

import jax
import jax.numpy as jnp
from jax import lax
from jax.experimental import pallas as pl
from jax.experimental.pallas import tpu as pltpu
from jax.sharding import Mesh
from jax.sharding import PartitionSpec as P

AXES = ("z", "y", "xl", "c", "xh")
BATCH = ("z", "y", "xl", "c")
NX, NY, NZ = 4, 4, 8
MESH = pl.DeviceIdType.MESH
ROWS = 128
HALF = 64
WIDE = 256
TILE = 1024
STEP = 32000.0
LOG2E = 1.4426950408889634
LN2 = 0.6931471805599453


def encode(x):
    top = jnp.max(jnp.abs(x), axis=0, keepdims=True)
    power = jnp.clip(jnp.floor(jnp.log(top) * LOG2E) + 1.0, -120.0, 120.0)
    value = jnp.round(x * (STEP * jnp.exp2(-power)))
    power = jnp.broadcast_to(power, (16, x.shape[1]))
    return (
        value.astype(jnp.int32).astype(jnp.int16),
        power.astype(jnp.int32).astype(jnp.int16),
    )


def decode(value, power):
    unit = jnp.exp2(power.astype(jnp.int32).astype(jnp.float32)[:1]) * (1.0 / STEP)
    return value.astype(jnp.int32).astype(jnp.float32) * unit


def to_lanes(column):
    return jnp.broadcast_to(column, (128, 128)).T[:1]


def to_rows(line):
    return jnp.broadcast_to(line, (128, 128)).T


def join(stack):
    high = jnp.max(stack, axis=0)
    return high + jnp.log(jnp.sum(jnp.exp2(stack - high[None]), axis=0)) * LOG2E


def nt(a, b):
    return lax.dot_general(a, b, (((1,), (1,)), ((), ())), preferred_element_type=jnp.float32)


def tn(a, b):
    return lax.dot_general(a, b, (((0,), (0,)), ((), ())), preferred_element_type=jnp.float32)


def kernel(
    q_ref, p_ref, pos_ref, gq_ref, gp_ref,
    Q, PT, S, W, posc, tmp, cmax, csum, rstat, cstat, rown, cown, rfin,
    XQ, GQ, SQ, RQ, SP, RP,
    relay, s_xq, r_xq, s_p, r_p, s_q, r_q, s_d, r_d, s_rs, r_rs, s_cs, r_cs,
    s_x, r_x, s_gp, r_gp, s_gq, r_gq,
):
    z, y, xl, c, xh = (lax.axis_index(a) for a in AXES)
    x = xh * 2 + xl
    factor = 1.0 / math.sqrt(2 * WIDE)

    def copy(src, dst, ssem, rsem, **where):
        return pltpu.make_async_remote_copy(
            src_ref=src, dst_ref=dst, send_sem=ssem, recv_sem=rsem,
            device_id=where, device_id_type=MESH,
        )

    def plane(k):
        tx, ty = lax.rem(x + k % 4, NX), lax.rem(y + k // 4, NY)
        return tx, ty, {"xh": tx // 2, "xl": lax.rem(tx, 2), "y": ty}

    def pillar(k):
        tz, tc = lax.rem(z + k // 2, NZ), lax.rem(c + k % 2, 2)
        return tz, tc, {"z": tz, "c": tc}

    near = (
        {"xh": lax.rem(x + 1, NX) // 2, "xl": 1 - xl},
        {"xh": lax.rem(x + 3, NX) // 2, "xl": 1 - xl},
        {"y": lax.rem(y + 1, NY)},
        {"y": lax.rem(y + 3, NY)},
        {"z": lax.rem(z + 1, NZ)},
        {"z": lax.rem(z + 7, NZ)},
        {"c": 1 - c},
    )
    barrier = pltpu.get_barrier_semaphore()
    for where in near:
        pl.semaphore_signal(barrier, inc=1, device_id=where, device_id_type=MESH)
    pl.semaphore_wait(barrier, len(near))
    for where in near[:2]:
        pl.semaphore_signal(relay, inc=1, device_id=where, device_id_type=MESH)

    slot_q = z * 2 + c
    half_rows = (
        pl.ds(pl.multiple_of(xh * HALF, HALF), HALF),
        pl.ds(pl.multiple_of((1 - xh) * HALF, HALF), HALF),
    )
    own_rows, other_rows = half_rows
    sends = []

    def start(cp):
        cp.start()
        sends.append(cp)

    def ring_items():
        a_of = lambda h, d: (h * HALF + (0 if d > 0 else 32), 32)
        own, rounds = (0, 0), ([], [], [], [])
        for d in (1, -1):
            for axis in (0, 1):
                turn = lambda o: o if axis == 0 else (o[1], o[0])
                first, second = (0, 1) if axis == 0 else (1, 0)
                rounds[0].append((axis, d, own, first * HALF, HALF, ()))
        for d in (1, -1):
            for axis in (0, 1):
                first, second = (0, 1) if axis == 0 else (1, 0)
                rounds[0].append((axis, d, own, second * HALF, HALF, ()))
        for d in (1, -1):
            for axis in (0, 1):
                turn = lambda o: o if axis == 0 else (o[1], o[0])
                first, second = (0, 1) if axis == 0 else (1, 0)
                rounds[1].append((axis, d, turn((-d, 0)), *a_of(first, d)))
        for e in (1, -1):
            for d in (1, -1):
                for axis in (0, 1):
                    turn = lambda o: o if axis == 0 else (o[1], o[0])
                    first, second = (0, 1) if axis == 0 else (1, 0)
                    rounds[1].append((axis, d, turn((0, e)), second * HALF, HALF))
        for d in (1, -1):
            for axis in (0, 1):
                turn = lambda o: o if axis == 0 else (o[1], o[0])
                first, second = (0, 1) if axis == 0 else (1, 0)
                rounds[1].append((axis, d, turn((-d, 0)), *a_of(second, d)))
        for d in (1, -1):
            for axis in (0, 1):
                turn = lambda o: o if axis == 0 else (o[1], o[0])
                first, second = (0, 1) if axis == 0 else (1, 0)
                rounds[2].append((axis, d, turn((0, 2)), second * HALF, HALF))
        for e in (1, -1):
            for d in (1, -1):
                for axis in (0, 1):
                    turn = lambda o: o if axis == 0 else (o[1], o[0])
                    first, second = (0, 1) if axis == 0 else (1, 0)
                    rounds[2].append((axis, d, turn((-d, e)), *a_of(second, d)))
        for d in (1, -1):
            for axis in (0, 1):
                turn = lambda o: o if axis == 0 else (o[1], o[0])
                first, second = (0, 1) if axis == 0 else (1, 0)
                rounds[3].append((axis, d, turn((-d, 2)), *a_of(second, d)))
        return [[(*item[:2], (item[2][0] % 4, item[2][1] % 4), *item[3:5]) for item in r] for r in rounds]

    rounds = ring_items()
    numbers = {item: n for n, item in enumerate(i for r in rounds for i in r)}
    arrived = set()

    def plane_copy(item, number, sender):
        axis, d, (dx, dy), first, rows = item
        if not sender:
            dx, dy = (dx - d, dy) if axis == 0 else (dx, dy - d)
        ox, oy = lax.rem(x + dx % 4, NX), lax.rem(y + dy % 4, NY)
        rows = pl.ds(first, rows)
        dst = PT.at[ox // 2, oy * 2 + lax.rem(ox, 2), rows]
        src = p_ref.at[rows] if item[2] == (0, 0) else dst
        return copy(src, dst, s_p.at[number], r_p.at[number], **near[axis * 2 + (d < 0)])

    def plane_wait(items):
        for item in items:
            if item not in arrived:
                arrived.add(item)
                plane_copy(item, numbers[item], False).wait_recv()

    def needs(item):
        axis, d, origin, first, rows = item
        found = []
        for other in numbers:
            oa, od, (ox, oy), of, orows = other
            got = ((ox - od) % 4, oy) if oa == 0 else (ox, (oy - od) % 4)
            if got == origin and of < first + rows and first < of + orows:
                found.append(other)
        return found

    def plane_round(n):
        for item in rounds[n]:
            if item[2] != (0, 0):
                plane_wait(needs(item))
            start(plane_copy(item, numbers[item], True))

    def ring_copy(d, step, part, sender):
        back = step - 1 if sender else step
        oz = lax.rem(z + (NZ - back * d) % NZ, NZ)
        rows = pl.ds((part % 2) * 32, 32)
        h = xh if part < 2 else 1 - xh
        dst = Q.at[h, oz * 2 + c, rows]
        src = dst
        if sender and step == 1 and part < 2:
            src = q_ref.at[pl.ds(pl.multiple_of(xh * HALF + part * 32, 32), 32)]
        number = ((d < 0) * 4 + step - 1) * 4 + part
        return copy(src, dst, s_q.at[number], r_q.at[number], **near[4 + (d < 0)])

    def carried(d, step, part):
        return step < 4 or part % 2 == (d < 0)

    def ring_send(step, group):
        for d in (1, -1):
            for part in (group * 2, group * 2 + 1):
                if carried(d, step, part):
                    start(ring_copy(d, step, part, True))

    def across(k, group, source):
        h = xh if group == 0 else 1 - xh
        oz = lax.rem(z + k, NZ)
        sc = c if source else 1 - c
        dst = Q.at[h, oz * 2 + sc]
        src = q_ref.at[own_rows] if k == 0 and group == 0 else Q.at[h, oz * 2 + c]
        return copy(src, dst, s_d.at[k, group], r_d.at[k, group], c=1 - c)

    def ring_wait(step, group):
        for d in (1, -1):
            for part in (group * 2, group * 2 + 1):
                if carried(d, step, part):
                    ring_copy(d, step, part, False).wait_recv()

    def pass_across(step, group):
        for k in {(NZ - step) % NZ, step % NZ}:
            start(across(k, group, True))

    exchange = copy(q_ref.at[other_rows], Q.at[xh, slot_q], s_xq, r_xq, xh=1 - xh)
    plane_round(0)
    ring_send(1, 0)
    pl.semaphore_wait(relay, 2)
    start(exchange)
    Q[xh, slot_q] = q_ref[own_rows, :]
    PT[xh, y * 2 + xl] = p_ref[...]
    start(across(0, 0, True))

    for s in range(16):
        line = (s // 2) * 16 + y * 4 + xl * 2 + s % 2
        tmp[...] = to_rows(pos_ref[pl.ds(line, 1), :])
        posc[s * HALF : (s + 1) * HALF] = tmp[own_rows, :]

    ring_wait(1, 0)
    ring_send(2, 0)
    plane_round(1)
    copy(q_ref.at[own_rows], Q.at[1 - xh, slot_q], s_xq, r_xq, xh=1 - xh).wait_recv()
    ring_send(1, 1)
    pass_across(1, 0)
    start(across(0, 1, True))
    ring_wait(2, 0)
    ring_send(3, 0)
    plane_round(2)
    ring_wait(1, 1)
    ring_send(2, 1)
    pass_across(2, 0)
    pass_across(1, 1)
    ring_wait(3, 0)
    ring_send(4, 0)
    plane_round(3)
    ring_wait(2, 1)
    ring_send(3, 1)
    pass_across(3, 0)
    pass_across(2, 1)
    ring_wait(4, 0)
    pass_across(4, 0)
    ring_wait(3, 1)
    ring_send(4, 1)
    pass_across(3, 1)
    for r in rounds:
        plane_wait(r)
    ring_wait(4, 1)
    pass_across(4, 1)
    for k in range(NZ):
        for group in range(2):
            across(k, group, False).wait_recv()

    def score(i, carry):
        rows = pl.ds(pl.multiple_of(i * 128, 128), 128)
        part = [
            nt(Q[h, pl.ds(i * 2, 2)].reshape(128, WIDE), PT[h].reshape(TILE, WIDE))
            for h in range(2)
        ]
        s = (part[0] + part[1]) * (factor * LOG2E)
        S[rows] = s
        high = jnp.max(s, axis=1, keepdims=True)
        total = jnp.sum(jnp.exp2(s - high), axis=1, keepdims=True)
        rown[pl.ds(i, 1)] = to_lanes(high + jnp.log(total) * LOG2E)
        chigh = jnp.max(s, axis=0, keepdims=True)
        cmax[pl.ds(i, 1)] = chigh
        csum[pl.ds(i, 1)] = jnp.sum(jnp.exp2(s - chigh), axis=0, keepdims=True)
        return carry

    lax.fori_loop(0, 8, score, 0)
    chigh = jnp.max(cmax[...], axis=0, keepdims=True)
    ctotal = jnp.sum(csum[...] * jnp.exp2(cmax[...] - chigh), axis=0, keepdims=True)
    cnorm = chigh + jnp.log(ctotal) * LOG2E
    for b in range(8):
        cown[b : b + 1] = cnorm[:, b * 128 : (b + 1) * 128]
    rstat[0] = rown[...]
    cstat[0] = cown[...]
    for k in range(1, 16):
        cp = copy(rown, rstat.at[k], s_rs.at[k], r_rs.at[k], **pillar(k)[2])
        cp.start()
        sends.append(cp)
        cp = copy(cown, cstat.at[k], s_cs.at[k], r_cs.at[k], **plane(k)[2])
        cp.start()
        sends.append(cp)
    for k in range(1, 16):
        copy(rown, rstat.at[k], s_rs.at[k], r_rs.at[k], **pillar(k)[2]).wait_recv()
        copy(cown, cstat.at[k], s_cs.at[k], r_cs.at[k], **plane(k)[2]).wait_recv()
    rown2 = join(rstat[...])
    cown2 = join(cstat[...])
    cmax[0:1] = jnp.concatenate([cown2[b : b + 1] for b in range(8)], axis=1)
    rfin[...] = rown2

    def weigh(i, carry):
        rows = pl.ds(pl.multiple_of(i * 128, 128), 128)
        rnorm = to_rows(rfin[pl.ds(i, 1), :])
        for b in range(8):
            cols = slice(b * 128, (b + 1) * 128)
            s = S[rows, cols]
            first = ((z * 4 + b // 2) * 2 + b % 2) * 2 + c
            ids = first * ROWS + lax.broadcasted_iota(jnp.int32, (128, 128), 1)
            match = jnp.where(posc[rows, :] == ids, 2.0, 0.0)
            w = jnp.exp2(s - rnorm) + jnp.exp2(s - cmax[0:1, cols]) - match
            W[rows, cols] = w.astype(jnp.bfloat16)
        return carry

    lax.fori_loop(0, 8, weigh, 0)

    for k in range(8):
        tz = lax.rem(z + k, NZ)
        rows = pl.ds(pl.multiple_of(tz * 128, 128), 128)
        for h in range(2):
            part = jnp.dot(W[rows, :], PT[h].reshape(TILE, WIDE), preferred_element_type=jnp.float32)
            tmp2 = part.reshape(2, HALF, WIDE)
            GQ[k, 0, h] = tmp2[0]
            GQ[k, 1, h] = tmp2[1]
        cp = copy(GQ.at[k, 1 - c], XQ.at[k], s_x.at[k], r_x.at[k], c=1 - c)
        cp.start()
        sends.append(cp)

    def send_queries(k):
        copy(GQ.at[k, 1 - c], XQ.at[k], s_x.at[k], r_x.at[k], c=1 - c).wait_recv()
        tz = lax.rem(z + k, NZ)
        for d in range(2):
            h = lax.rem(xh + d, 2)
            value, power = encode(GQ[k, c, h] + XQ[k, h])
            if k == 0 and d == 0:
                RQ[0, 0, 0:HALF] = value
                RQ[0, 0, HALF:] = power
                continue
            SQ[k, d, 0:HALF] = value
            SQ[k, d, HALF:] = power
            cp = copy(SQ.at[k, d], RQ.at[k, d], s_gq.at[k, d], r_gq.at[k, d], z=tz, xh=h)
            cp.start()
            sends.append(cp)

    order = [k for k in range(1, 16)] + [0]
    for n, k in enumerate(order):
        tx, ty, where = plane(k)
        cols = pl.ds(pl.multiple_of((ty * 2 + lax.rem(tx, 2)) * 128, 128), 128)
        value, power = encode(tn(W[:, cols], Q[tx // 2].reshape(TILE, WIDE)))
        if k == 0:
            RP[0, 0:ROWS] = value
            RP[0, ROWS:] = power
        else:
            SP[k, 0:ROWS] = value
            SP[k, ROWS:] = power
            cp = copy(SP.at[k], RP.at[k], s_gp.at[k], r_gp.at[k], **where)
            cp.start()
            sends.append(cp)
        if n % 2 == 1:
            send_queries((n // 2 + 1) % 8)

    total = jnp.zeros((ROWS, WIDE), jnp.float32)
    for k in range(16):
        if k:
            copy(SP.at[k], RP.at[k], s_gp.at[k], r_gp.at[k], **plane(k)[2]).wait_recv()
        total = total + decode(RP[k, 0:ROWS], RP[k, ROWS:])
    gp_ref[...] = total * factor
    for d in range(2):
        total = jnp.zeros((HALF, WIDE), jnp.float32)
        for k in range(8):
            if k or d:
                copy(SQ.at[k, d], RQ.at[k, d], s_gq.at[k, d], r_gq.at[k, d], z=lax.rem(z + k, NZ)).wait_recv()
            total = total + decode(RQ[k, d, 0:HALF], RQ[k, d, HALF:])
        gq_ref[(own_rows, other_rows)[d], :] = total * factor
    for cp in sends:
        cp.wait_send()


def local(queries, passages, positives):
    dma = pltpu.SemaphoreType.DMA
    vmem = pl.BlockSpec(memory_space=pltpu.VMEM)
    out = jax.ShapeDtypeStruct((ROWS, WIDE), jnp.float32)
    bf16, f32, i16 = jnp.bfloat16, jnp.float32, jnp.int16
    return pl.pallas_call(
        kernel,
        out_shape=(out, out),
        in_specs=[vmem] * 3,
        out_specs=(vmem, vmem),
        scratch_shapes=[
            pltpu.VMEM((2, 16, HALF, WIDE), bf16),
            pltpu.VMEM((2, 8, ROWS, WIDE), bf16),
            pltpu.VMEM((TILE, TILE), f32),
            pltpu.VMEM((TILE, TILE), bf16),
            pltpu.VMEM((TILE, 128), jnp.int32),
            pltpu.VMEM((128, 128), jnp.int32),
            pltpu.VMEM((8, TILE), f32),
            pltpu.VMEM((8, TILE), f32),
            pltpu.VMEM((16, 8, 128), f32),
            pltpu.VMEM((16, 8, 128), f32),
            pltpu.VMEM((8, 128), f32),
            pltpu.VMEM((8, 128), f32),
            pltpu.VMEM((8, 128), f32),
            pltpu.VMEM((8, 2, HALF, WIDE), f32),
            pltpu.VMEM((8, 2, 2, HALF, WIDE), f32),
            pltpu.VMEM((8, 2, HALF + 16, WIDE), i16),
            pltpu.VMEM((8, 2, HALF + 16, WIDE), i16),
            pltpu.VMEM((16, ROWS + 16, WIDE), i16),
            pltpu.VMEM((16, ROWS + 16, WIDE), i16),
            pltpu.SemaphoreType.REGULAR,
            dma, dma,
            dma((40,)), dma((40,)),
            dma((32,)), dma((32,)),
            dma((8, 2)), dma((8, 2)),
            dma((16,)), dma((16,)),
            dma((16,)), dma((16,)),
            dma((8,)), dma((8,)),
            dma((16,)), dma((16,)),
            dma((8, 2)), dma((8, 2)),
        ],
        compiler_params=pltpu.CompilerParams(
            collective_id=0, has_side_effects=True, vmem_limit_bytes=60 * 1024 * 1024
        ),
    )(queries, passages, positives.reshape(128, 128))


def solution(mesh):
    split = Mesh(
        mesh.devices.reshape(NZ, NY, 2, 2, mesh.shape["rep"]),
        AXES,
    )
    return jax.shard_map(
        local,
        mesh=split,
        in_specs=(P(BATCH, "xh"), P(BATCH, "xh"), P()),
        out_specs=(P(BATCH, "xh"), P(BATCH, "xh")),
        check_vma=False,
    )
```

```python
import math

import jax
import jax.numpy as jnp
from jax import lax
from jax.experimental import pallas as pl
from jax.experimental.pallas import tpu as pltpu
from jax.sharding import Mesh
from jax.sharding import PartitionSpec as P

AXES = ("z", "y", "xl", "c", "xh")
BATCH = ("z", "y", "xl", "c")
NX, NY, NZ = 4, 4, 8
MESH = pl.DeviceIdType.MESH
ROWS = 128
HALF = 64
WIDE = 256
TILE = 1024
STEP = 32000.0
LOG2E = 1.4426950408889634
LN2 = 0.6931471805599453


def encode(x):
    top = jnp.max(jnp.abs(x), axis=0, keepdims=True)
    power = jnp.clip(jnp.floor(jnp.log(top) * LOG2E) + 1.0, -120.0, 120.0)
    value = jnp.round(x * (STEP * jnp.exp2(-power)))
    power = jnp.broadcast_to(power, (16, x.shape[1]))
    return (
        value.astype(jnp.int32).astype(jnp.int16),
        power.astype(jnp.int32).astype(jnp.int16),
    )


def decode(value, power):
    unit = jnp.exp2(power.astype(jnp.int32).astype(jnp.float32)[:1]) * (1.0 / STEP)
    return value.astype(jnp.int32).astype(jnp.float32) * unit


def to_lanes(column):
    return jnp.broadcast_to(column, (128, 128)).T[:1]


def to_rows(line):
    return jnp.broadcast_to(line, (128, 128)).T


def join(stack):
    high = jnp.max(stack, axis=0)
    return high + jnp.log(jnp.sum(jnp.exp2(stack - high[None]), axis=0)) * LOG2E


def nt(a, b):
    return lax.dot_general(a, b, (((1,), (1,)), ((), ())), preferred_element_type=jnp.float32)


def tn(a, b):
    return lax.dot_general(a, b, (((0,), (0,)), ((), ())), preferred_element_type=jnp.float32)


def kernel(
    q_ref, p_ref, pos_ref, gq_ref, gp_ref,
    Q, PT, S, W, posc, tmp, cmax, csum, rstat, cstat, rown, cown, rfin,
    XQ, GQ, SQ, RQ, SP, RP,
    s_xq, r_xq, s_p, r_p, s_q, r_q, s_d, r_d, s_rs, r_rs, s_cs, r_cs,
    s_x, r_x, s_gp, r_gp, s_gq, r_gq,
):
    z, y, xl, c, xh = (lax.axis_index(a) for a in AXES)
    x = xh * 2 + xl
    factor = 1.0 / math.sqrt(2 * WIDE)

    def copy(src, dst, ssem, rsem, **where):
        return pltpu.make_async_remote_copy(
            src_ref=src, dst_ref=dst, send_sem=ssem, recv_sem=rsem,
            device_id=where, device_id_type=MESH,
        )

    def plane(k):
        tx, ty = lax.rem(x + k % 4, NX), lax.rem(y + k // 4, NY)
        return tx, ty, {"xh": tx // 2, "xl": lax.rem(tx, 2), "y": ty}

    def pillar(k):
        tz, tc = lax.rem(z + k // 2, NZ), lax.rem(c + k % 2, 2)
        return tz, tc, {"z": tz, "c": tc}

    def along(axis, e):
        if axis == 0:
            t = lax.rem(x + e, NX)
            return {"xh": t // 2, "xl": lax.rem(t, 2)}
        return {"y": lax.rem(y + e, NY)} if axis == 1 else {"z": lax.rem(z + e, NZ)}

    barrier = pltpu.get_barrier_semaphore()
    near = [along(axis, e) for e in (1, 2, 3) for axis in (0, 1)]
    near += [along(2, e) for e in (1, 7, 2, 6)] + [{"c": 1 - c}]
    for where in near:
        pl.semaphore_signal(barrier, inc=1, device_id=where, device_id_type=MESH)
    pl.semaphore_wait(barrier, len(near))

    slot_q = z * 2 + c
    slot_p = y * 2 + xl
    own_rows = pl.ds(pl.multiple_of(xh * HALF, HALF), HALF)
    other_rows = pl.ds(pl.multiple_of((1 - xh) * HALF, HALF), HALF)
    sends = []

    def start(cp):
        cp.start()
        sends.append(cp)

    def plane_copy(half, phase, e, f, sender):
        first, second = (0, 1) if half == 0 else (1, 0)
        off = [0, 0]
        if phase:
            off[first] -= f
        if not sender:
            off[second if phase else first] -= e
        ox, oy = lax.rem(x + off[0] % 4, NX), lax.rem(y + off[1] % 4, NY)
        rows = pl.ds(half * HALF, HALF)
        dst = PT.at[ox // 2, oy * 2 + lax.rem(ox, 2), rows]
        src = p_ref.at[rows] if sender and f == 0 else dst
        at = (half, phase * (f + 1), e)
        return copy(src, dst, s_p.at[at], r_p.at[at], **along(second if phase else first, e))

    def ring_copy(group, hop, back, e, rows, number, sender):
        oz = lax.rem(z + (16 - back - (0 if sender else e)) % NZ, NZ)
        h = xh if group == 0 else 1 - xh
        dst = Q.at[h, oz * 2 + c, rows]
        src = dst
        if sender and back == 0 and group == 0:
            src = q_ref.at[own_rows]
        at = (group, number)
        return copy(src, dst, s_q.at[at], r_q.at[at], **along(2, e % NZ))

    whole, low, high = pl.ds(0, HALF), pl.ds(0, 32), pl.ds(32, 32)
    hops = [(0, 0, 2, whole), (0, 0, -2, whole), (0, 0, 1, whole), (0, 0, -1, whole),
            (1, 2, 2, low), (1, -2, -2, high), (1, 2, 1, whole), (1, -2, -1, whole)]

    def ring(group, n, sender):
        return ring_copy(group, *hops[n], n, sender)

    def across(k, group, source):
        h = xh if group == 0 else 1 - xh
        oz = lax.rem(z + k, NZ)
        dst = Q.at[h, oz * 2 + (c if source else 1 - c)]
        src = q_ref.at[own_rows] if source and isinstance(k, int) and k == 0 and group == 0 else Q.at[h, oz * 2 + c]
        return copy(src, dst, s_d.at[k, group], r_d.at[k, group], c=1 - c)

    def ring_take(group, n, *ks):
        for m in n:
            ring(group, m, False).wait_recv()
        for k in ks:
            start(across(k, group, True))

    start(copy(q_ref.at[other_rows], Q.at[xh, slot_q], s_xq, r_xq, **along(0, 2)))
    for e in (2, 1, 3):
        for half in range(2):
            start(plane_copy(half, 0, e, 0, True))
    for n in range(4):
        start(ring(0, n, True))
    for e in (2, 1, 3):
        for half in range(2):
            start(plane_copy(half, 1, e, 0, True))
    start(across(0, 0, True))
    Q[xh, slot_q] = q_ref[own_rows, :]
    PT[xh, slot_p] = p_ref[...]

    for s in range(16):
        line = (s // 2) * 16 + y * 4 + xl * 2 + s % 2
        tmp[...] = to_rows(pos_ref[pl.ds(line, 1), :])
        posc[s * HALF : (s + 1) * HALF] = tmp[own_rows, :]

    def plane_pass(f):
        for half in range(2):
            plane_copy(half, 0, f, 0, False).wait_recv()
            for e in (2, 1, 3):
                start(plane_copy(half, 1, e, f, True))

    plane_pass(1)
    plane_pass(3)
    copy(q_ref.at[own_rows], Q.at[1 - xh, slot_q], s_xq, r_xq, **along(0, 2)).wait_recv()
    for n in range(4):
        start(ring(1, n, True))
    start(across(0, 1, True))
    plane_pass(2)
    ring_take(0, (0,), 6)
    start(ring(0, 4, True))
    start(ring(0, 6, True))
    ring_take(0, (1,), 2)
    start(ring(0, 5, True))
    start(ring(0, 7, True))
    ring_take(0, (2,), 7)
    ring_take(0, (3,), 1)
    ring_take(1, (0,), 6)
    start(ring(1, 4, True))
    start(ring(1, 6, True))
    ring_take(1, (1,), 2)
    start(ring(1, 5, True))
    start(ring(1, 7, True))
    ring_take(1, (2,), 7)
    ring_take(1, (3,), 1)
    for half in range(2):
        for f in range(4):
            for e in (1, 2, 3):
                plane_copy(half, 1, e, f, False).wait_recv()
    ring_take(0, (6,), 5)
    ring_take(0, (7,), 3)
    ring_take(0, (4, 5), 4)

    def score(n, carry):
        k = lax.rem(lax.select(lax.rem(n, 2) == 1, (n + 1) // 2, NZ - n // 2), NZ)
        i = lax.rem(z + k, NZ)
        for group in range(2):
            across(k, group, False).wait_recv()
        rows = pl.ds(pl.multiple_of(i * 128, 128), 128)
        part = [
            nt(Q[h, pl.ds(i * 2, 2)].reshape(128, WIDE), PT[h].reshape(TILE, WIDE))
            for h in range(2)
        ]
        s = (part[0] + part[1]) * (factor * LOG2E)
        S[rows] = s
        high = jnp.max(s, axis=1, keepdims=True)
        total = jnp.sum(jnp.exp2(s - high), axis=1, keepdims=True)
        rown[pl.ds(i, 1)] = to_lanes(high + jnp.log(total) * LOG2E)
        chigh = jnp.max(s, axis=0, keepdims=True)
        cmax[pl.ds(n, 1)] = chigh
        csum[pl.ds(n, 1)] = jnp.sum(jnp.exp2(s - chigh), axis=0, keepdims=True)
        return carry

    lax.fori_loop(0, 3, score, 0)
    ring_take(1, (6,), 5)
    ring_take(1, (7,), 3)
    ring_take(1, (4, 5), 4)
    lax.fori_loop(3, 8, score, 0)
    chigh = jnp.max(cmax[...], axis=0, keepdims=True)
    ctotal = jnp.sum(csum[...] * jnp.exp2(cmax[...] - chigh), axis=0, keepdims=True)
    cnorm = chigh + jnp.log(ctotal) * LOG2E
    for b in range(8):
        cown[b : b + 1] = cnorm[:, b * 128 : (b + 1) * 128]
    rstat[0] = rown[...]
    cstat[0] = cown[...]
    for k in range(1, 16):
        cp = copy(rown, rstat.at[k], s_rs.at[k], r_rs.at[k], **pillar(k)[2])
        cp.start()
        sends.append(cp)
        cp = copy(cown, cstat.at[k], s_cs.at[k], r_cs.at[k], **plane(k)[2])
        cp.start()
        sends.append(cp)
    for k in range(1, 16):
        copy(rown, rstat.at[k], s_rs.at[k], r_rs.at[k], **pillar(k)[2]).wait_recv()
        copy(cown, cstat.at[k], s_cs.at[k], r_cs.at[k], **plane(k)[2]).wait_recv()
    rown2 = join(rstat[...])
    cown2 = join(cstat[...])
    cmax[0:1] = jnp.concatenate([cown2[b : b + 1] for b in range(8)], axis=1)
    rfin[...] = rown2

    def weigh(i, carry):
        rows = pl.ds(pl.multiple_of(i * 128, 128), 128)
        rnorm = to_rows(rfin[pl.ds(i, 1), :])
        for b in range(8):
            cols = slice(b * 128, (b + 1) * 128)
            s = S[rows, cols]
            first = ((z * 4 + b // 2) * 2 + b % 2) * 2 + c
            ids = first * ROWS + lax.broadcasted_iota(jnp.int32, (128, 128), 1)
            match = jnp.where(posc[rows, :] == ids, 2.0, 0.0)
            w = jnp.exp2(s - rnorm) + jnp.exp2(s - cmax[0:1, cols]) - match
            W[rows, cols] = w.astype(jnp.bfloat16)
        return carry

    lax.fori_loop(0, 8, weigh, 0)

    for k in range(8):
        tz = lax.rem(z + k, NZ)
        rows = pl.ds(pl.multiple_of(tz * 128, 128), 128)
        for h in range(2):
            part = jnp.dot(W[rows, :], PT[h].reshape(TILE, WIDE), preferred_element_type=jnp.float32)
            tmp2 = part.reshape(2, HALF, WIDE)
            GQ[k, 0, h] = tmp2[0]
            GQ[k, 1, h] = tmp2[1]
        cp = copy(GQ.at[k, 1 - c], XQ.at[k], s_x.at[k], r_x.at[k], c=1 - c)
        cp.start()
        sends.append(cp)

    def send_queries(k):
        copy(GQ.at[k, 1 - c], XQ.at[k], s_x.at[k], r_x.at[k], c=1 - c).wait_recv()
        tz = lax.rem(z + k, NZ)
        for d in range(2):
            h = lax.rem(xh + d, 2)
            value, power = encode(GQ[k, c, h] + XQ[k, h])
            if k == 0 and d == 0:
                RQ[0, 0, 0:HALF] = value
                RQ[0, 0, HALF:] = power
                continue
            SQ[k, d, 0:HALF] = value
            SQ[k, d, HALF:] = power
            cp = copy(SQ.at[k, d], RQ.at[k, d], s_gq.at[k, d], r_gq.at[k, d], z=tz, xh=h)
            cp.start()
            sends.append(cp)

    order = [k for k in range(1, 16)] + [0]
    for n, k in enumerate(order):
        tx, ty, where = plane(k)
        cols = pl.ds(pl.multiple_of((ty * 2 + lax.rem(tx, 2)) * 128, 128), 128)
        value, power = encode(tn(W[:, cols], Q[tx // 2].reshape(TILE, WIDE)))
        if k == 0:
            RP[0, 0:ROWS] = value
            RP[0, ROWS:] = power
        else:
            SP[k, 0:ROWS] = value
            SP[k, ROWS:] = power
            cp = copy(SP.at[k], RP.at[k], s_gp.at[k], r_gp.at[k], **where)
            cp.start()
            sends.append(cp)
        if n % 2 == 1:
            send_queries((n // 2 + 1) % 8)

    total = jnp.zeros((ROWS, WIDE), jnp.float32)
    for k in range(16):
        if k:
            copy(SP.at[k], RP.at[k], s_gp.at[k], r_gp.at[k], **plane(k)[2]).wait_recv()
        total = total + decode(RP[k, 0:ROWS], RP[k, ROWS:])
    gp_ref[...] = total * factor
    for d in range(2):
        total = jnp.zeros((HALF, WIDE), jnp.float32)
        for k in range(8):
            if k or d:
                copy(SQ.at[k, d], RQ.at[k, d], s_gq.at[k, d], r_gq.at[k, d], z=lax.rem(z + k, NZ)).wait_recv()
            total = total + decode(RQ[k, d, 0:HALF], RQ[k, d, HALF:])
        gq_ref[(own_rows, other_rows)[d], :] = total * factor
    for cp in sends:
        cp.wait_send()


def local(queries, passages, positives):
    dma = pltpu.SemaphoreType.DMA
    vmem = pl.BlockSpec(memory_space=pltpu.VMEM)
    out = jax.ShapeDtypeStruct((ROWS, WIDE), jnp.float32)
    bf16, f32, i16 = jnp.bfloat16, jnp.float32, jnp.int16
    return pl.pallas_call(
        kernel,
        out_shape=(out, out),
        in_specs=[vmem] * 3,
        out_specs=(vmem, vmem),
        scratch_shapes=[
            pltpu.VMEM((2, 16, HALF, WIDE), bf16),
            pltpu.VMEM((2, 8, ROWS, WIDE), bf16),
            pltpu.VMEM((TILE, TILE), f32),
            pltpu.VMEM((TILE, TILE), bf16),
            pltpu.VMEM((TILE, 128), jnp.int32),
            pltpu.VMEM((128, 128), jnp.int32),
            pltpu.VMEM((8, TILE), f32),
            pltpu.VMEM((8, TILE), f32),
            pltpu.VMEM((16, 8, 128), f32),
            pltpu.VMEM((16, 8, 128), f32),
            pltpu.VMEM((8, 128), f32),
            pltpu.VMEM((8, 128), f32),
            pltpu.VMEM((8, 128), f32),
            pltpu.VMEM((8, 2, HALF, WIDE), f32),
            pltpu.VMEM((8, 2, 2, HALF, WIDE), f32),
            pltpu.VMEM((8, 2, HALF + 16, WIDE), i16),
            pltpu.VMEM((8, 2, HALF + 16, WIDE), i16),
            pltpu.VMEM((16, ROWS + 16, WIDE), i16),
            pltpu.VMEM((16, ROWS + 16, WIDE), i16),
            dma, dma,
            dma((2, 5, 4)), dma((2, 5, 4)),
            dma((2, 8)), dma((2, 8)),
            dma((8, 2)), dma((8, 2)),
            dma((16,)), dma((16,)),
            dma((16,)), dma((16,)),
            dma((8,)), dma((8,)),
            dma((16,)), dma((16,)),
            dma((8, 2)), dma((8, 2)),
        ],
        compiler_params=pltpu.CompilerParams(
            collective_id=0, has_side_effects=True, vmem_limit_bytes=60 * 1024 * 1024
        ),
    )(queries, passages, positives.reshape(128, 128))


def solution(mesh):
    split = Mesh(
        mesh.devices.reshape(NZ, NY, 2, 2, mesh.shape["rep"]),
        AXES,
    )
    return jax.shard_map(
        local,
        mesh=split,
        in_specs=(P(BATCH, "xh"), P(BATCH, "xh"), P()),
        out_specs=(P(BATCH, "xh"), P(BATCH, "xh")),
        check_vma=False,
    )
```

```python
import math

import jax
import jax.numpy as jnp
from jax import lax
from jax.experimental import pallas as pl
from jax.experimental.pallas import tpu as pltpu
from jax.sharding import Mesh
from jax.sharding import PartitionSpec as P

AXES = ("z", "y", "xl", "c", "xh")
BATCH = ("z", "y", "xl", "c")
NX, NY, NZ = 4, 4, 8
MESH = pl.DeviceIdType.MESH
ROWS = 128
HALF = 64
WIDE = 256
TILE = 1024
FIRST = 64
STEP = 32000.0
LOG2E = 1.4426950408889634
LN2 = 0.6931471805599453


def put(ref, x):
    rows = x.shape[0]
    top = jnp.max(jnp.abs(x), axis=0, keepdims=True)
    power = jnp.clip(jnp.floor(jnp.log(top) * LOG2E) + 1.0, -120.0, 120.0)
    value = jnp.round(x * (STEP * jnp.exp2(-power))).astype(jnp.int32).astype(jnp.int16)
    ref[0:rows] = value[:, :128]
    ref[rows : 2 * rows] = value[:, 128:]
    both = [jnp.broadcast_to(power[:, at : at + 128], (8, 128)) for at in (0, 128)]
    ref[2 * rows :] = jnp.concatenate(both, axis=0).astype(jnp.int32).astype(jnp.int16)


def take(ref):
    rows = (ref.shape[0] - 16) // 2
    unit = jnp.exp2(ref[2 * rows :].astype(jnp.int32).astype(jnp.float32)) * (1.0 / STEP)
    value = ref[0 : 2 * rows].astype(jnp.int32).astype(jnp.float32)
    return jnp.concatenate([value[:rows] * unit[0:1], value[rows:] * unit[8:9]], axis=1)


def to_lanes(column):
    return jnp.broadcast_to(column, (128, 128)).T[:1]


def to_rows(line):
    return jnp.broadcast_to(line, (128, 128)).T


def join(stack):
    high = jnp.max(stack, axis=0)
    return high + jnp.log(jnp.sum(jnp.exp2(stack - high[None]), axis=0)) * LOG2E


def nt(a, b):
    return lax.dot_general(a, b, (((1,), (1,)), ((), ())), preferred_element_type=jnp.float32)


def tn(a, b):
    return lax.dot_general(a, b, (((0,), (0,)), ((), ())), preferred_element_type=jnp.float32)


def kernel(
    q_ref, p_ref, pos_ref, gq_ref, gp_ref,
    Q, PT, S, W, posc, tmp, cmax, csum, rstat, cstat, rown, cown, rfin,
    XQ, GQ, SQ, RQ, OWN1, OWN2, SP1, SP2, RP1, RP2, SS1, SS2, RS1, RS2,
    s_xq, r_xq, s_p, r_p, s_q, r_q, s_d, r_d, s_rs, r_rs, s_cs, r_cs,
    s_x, r_x, s_gp, r_gp, s_gq, r_gq,
):
    z, y, xl, c, xh = (lax.axis_index(a) for a in AXES)
    x = xh * 2 + xl
    factor = 1.0 / math.sqrt(2 * WIDE)

    def copy(src, dst, ssem, rsem, **where):
        return pltpu.make_async_remote_copy(
            src_ref=src, dst_ref=dst, send_sem=ssem, recv_sem=rsem,
            device_id=where, device_id_type=MESH,
        )

    def plane(k):
        tx, ty = lax.rem(x + k % 4, NX), lax.rem(y + k // 4, NY)
        return tx, ty, {"xh": tx // 2, "xl": lax.rem(tx, 2), "y": ty}

    def pillar(k):
        tz, tc = lax.rem(z + k // 2, NZ), lax.rem(c + k % 2, 2)
        return tz, tc, {"z": tz, "c": tc}

    def along(axis, e):
        if axis == 0:
            t = lax.rem(x + e, NX)
            return {"xh": t // 2, "xl": lax.rem(t, 2)}
        return {"y": lax.rem(y + e, NY)} if axis == 1 else {"z": lax.rem(z + e, NZ)}

    barrier = pltpu.get_barrier_semaphore()
    near = [along(axis, e) for e in (1, 2, 3) for axis in (0, 1)]
    near += [along(2, e) for e in (1, 7, 2, 6)] + [{"c": 1 - c}]
    for where in near:
        pl.semaphore_signal(barrier, inc=1, device_id=where, device_id_type=MESH)
    pl.semaphore_wait(barrier, len(near))

    slot_q = z * 2 + c
    slot_p = y * 2 + xl
    own_rows = pl.ds(pl.multiple_of(xh * HALF, HALF), HALF)
    other_rows = pl.ds(pl.multiple_of((1 - xh) * HALF, HALF), HALF)
    sends = []

    def start(cp):
        cp.start()
        sends.append(cp)

    def plane_copy(half, phase, e, f, sender):
        first, second = (0, 1) if half == 0 else (1, 0)
        off = [0, 0]
        if phase:
            off[first] -= f
        if not sender:
            off[second if phase else first] -= e
        ox, oy = lax.rem(x + off[0] % 4, NX), lax.rem(y + off[1] % 4, NY)
        rows = pl.ds(half * HALF, HALF)
        dst = PT.at[ox // 2, oy * 2 + lax.rem(ox, 2), rows]
        src = p_ref.at[rows] if sender and f == 0 else dst
        at = (half, phase * (f + 1), e)
        return copy(src, dst, s_p.at[at], r_p.at[at], **along(second if phase else first, e))

    def ring_copy(group, hop, back, e, rows, number, sender):
        oz = lax.rem(z + (16 - back - (0 if sender else e)) % NZ, NZ)
        h = xh if group == 0 else 1 - xh
        dst = Q.at[h, oz * 2 + c, rows]
        src = dst
        if sender and back == 0 and group == 0:
            src = q_ref.at[own_rows]
        at = (group, number)
        return copy(src, dst, s_q.at[at], r_q.at[at], **along(2, e % NZ))

    whole, low, high = pl.ds(0, HALF), pl.ds(0, 32), pl.ds(32, 32)
    hops = [(0, 0, 2, whole), (0, 0, -2, whole), (0, 0, 1, whole), (0, 0, -1, whole),
            (1, 2, 2, low), (1, -2, -2, high), (1, 2, 1, whole), (1, -2, -1, whole)]

    def ring(group, n, sender):
        return ring_copy(group, *hops[n], n, sender)

    def across(k, group, source):
        h = xh if group == 0 else 1 - xh
        oz = lax.rem(z + k, NZ)
        dst = Q.at[h, oz * 2 + (c if source else 1 - c)]
        src = q_ref.at[own_rows] if source and isinstance(k, int) and k == 0 and group == 0 else Q.at[h, oz * 2 + c]
        return copy(src, dst, s_d.at[k, group], r_d.at[k, group], c=1 - c)

    def ring_take(group, n, *ks):
        for m in n:
            ring(group, m, False).wait_recv()
        for k in ks:
            start(across(k, group, True))

    start(copy(q_ref.at[other_rows], Q.at[xh, slot_q], s_xq, r_xq, **along(0, 2)))
    for e in (2, 1, 3):
        for half in range(2):
            start(plane_copy(half, 0, e, 0, True))
    for n in range(4):
        start(ring(0, n, True))
    for e in (2, 1, 3):
        for half in range(2):
            start(plane_copy(half, 1, e, 0, True))
    start(across(0, 0, True))
    Q[xh, slot_q] = q_ref[own_rows, :]
    PT[xh, slot_p] = p_ref[...]

    for s in range(16):
        line = (s // 2) * 16 + y * 4 + xl * 2 + s % 2
        tmp[...] = to_rows(pos_ref[pl.ds(line, 1), :])
        posc[s * HALF : (s + 1) * HALF] = tmp[own_rows, :]

    def plane_pass(f):
        for half in range(2):
            plane_copy(half, 0, f, 0, False).wait_recv()
            for e in (2, 1, 3):
                start(plane_copy(half, 1, e, f, True))

    plane_pass(1)
    plane_pass(3)
    copy(q_ref.at[own_rows], Q.at[1 - xh, slot_q], s_xq, r_xq, **along(0, 2)).wait_recv()
    for n in range(4):
        start(ring(1, n, True))
    start(across(0, 1, True))
    plane_pass(2)
    ring_take(0, (0,), 6)
    start(ring(0, 4, True))
    start(ring(0, 6, True))
    ring_take(0, (1,), 2)
    start(ring(0, 5, True))
    start(ring(0, 7, True))
    ring_take(0, (2,), 7)
    ring_take(0, (3,), 1)
    ring_take(1, (0,), 6)
    start(ring(1, 4, True))
    start(ring(1, 6, True))
    ring_take(1, (1,), 2)
    start(ring(1, 5, True))
    start(ring(1, 7, True))
    ring_take(1, (2,), 7)
    ring_take(1, (3,), 1)
    for half in range(2):
        for f in range(4):
            for e in (1, 2, 3):
                plane_copy(half, 1, e, f, False).wait_recv()
    ring_take(0, (6,), 5)
    ring_take(0, (7,), 3)
    ring_take(0, (4, 5), 4)

    def score(n, carry):
        k = lax.rem(lax.select(lax.rem(n, 2) == 1, (n + 1) // 2, NZ - n // 2), NZ)
        i = lax.rem(z + k, NZ)
        for group in range(2):
            across(k, group, False).wait_recv()
        rows = pl.ds(pl.multiple_of(i * 128, 128), 128)
        part = [
            nt(Q[h, pl.ds(i * 2, 2)].reshape(128, WIDE), PT[h].reshape(TILE, WIDE))
            for h in range(2)
        ]
        s = (part[0] + part[1]) * (factor * LOG2E)
        S[rows] = s
        high = jnp.max(s, axis=1, keepdims=True)
        total = jnp.sum(jnp.exp2(s - high), axis=1, keepdims=True)
        rown[pl.ds(i, 1)] = to_lanes(high + jnp.log(total) * LOG2E)
        chigh = jnp.max(s, axis=0, keepdims=True)
        cmax[pl.ds(n, 1)] = chigh
        csum[pl.ds(n, 1)] = jnp.sum(jnp.exp2(s - chigh), axis=0, keepdims=True)
        return carry

    lax.fori_loop(0, 3, score, 0)
    ring_take(1, (6,), 5)
    ring_take(1, (7,), 3)
    ring_take(1, (4, 5), 4)
    lax.fori_loop(3, 8, score, 0)
    chigh = jnp.max(cmax[...], axis=0, keepdims=True)
    ctotal = jnp.sum(csum[...] * jnp.exp2(cmax[...] - chigh), axis=0, keepdims=True)
    cnorm = chigh + jnp.log(ctotal) * LOG2E
    for b in range(8):
        cown[b : b + 1] = cnorm[:, b * 128 : (b + 1) * 128]
    rstat[0] = rown[...]
    cstat[0] = cown[...]
    for k in range(1, 16):
        cp = copy(rown, rstat.at[k], s_rs.at[k], r_rs.at[k], **pillar(k)[2])
        cp.start()
        sends.append(cp)
        cp = copy(cown, cstat.at[k], s_cs.at[k], r_cs.at[k], **plane(k)[2])
        cp.start()
        sends.append(cp)
    for k in range(1, 16):
        copy(rown, rstat.at[k], s_rs.at[k], r_rs.at[k], **pillar(k)[2]).wait_recv()
        copy(cown, cstat.at[k], s_cs.at[k], r_cs.at[k], **plane(k)[2]).wait_recv()
    rown2 = join(rstat[...])
    cown2 = join(cstat[...])
    cmax[0:1] = jnp.concatenate([cown2[b : b + 1] for b in range(8)], axis=1)
    rfin[...] = rown2

    def weigh(i, carry):
        rows = pl.ds(pl.multiple_of(i * 128, 128), 128)
        rnorm = to_rows(rfin[pl.ds(i, 1), :])
        for b in range(8):
            cols = slice(b * 128, (b + 1) * 128)
            s = S[rows, cols]
            first = ((z * 4 + b // 2) * 2 + b % 2) * 2 + c
            ids = first * ROWS + lax.broadcasted_iota(jnp.int32, (128, 128), 1)
            match = jnp.where(posc[rows, :] == ids, 2.0, 0.0)
            w = jnp.exp2(s - rnorm) + jnp.exp2(s - cmax[0:1, cols]) - match
            W[rows, cols] = w.astype(jnp.bfloat16)
        return carry

    lax.fori_loop(0, 8, weigh, 0)

    def query_product(k):
        rows = pl.ds(pl.multiple_of(lax.rem(z + k, NZ) * 128, 128), 128)
        for h in range(2):
            part = jnp.dot(W[rows, :], PT[h].reshape(TILE, WIDE), preferred_element_type=jnp.float32)
            part = part.reshape(2, HALF, WIDE)
            GQ[k, 0, h] = part[0]
            GQ[k, 1, h] = part[1]
        start(swap(k))

    def swap(k):
        return copy(GQ.at[k, 1 - c], XQ.at[k], s_x.at[k], r_x.at[k], c=1 - c)

    def side(d):
        return xh if d == 0 else 1 - xh

    def query_sum(k, d):
        return GQ[k, c, side(d)] + XQ[k, side(d)]

    legs = [(4, 0, 2), (4, 1, -2), (3, 0, 1), (3, 1, 1), (5, 0, -1), (5, 1, -1),
            (2, 0, 2), (2, 1, 2), (6, 0, -2), (6, 1, -2), (1, 0, 1), (1, 1, 1), (7, 0, -1), (7, 1, -1), (0, 1, 0)]

    def leg(n):
        k, d, e = legs[n]
        where = along(2, e % NZ) if e else {}
        if n >= 6 and d:
            where["xh"] = 1 - xh
        return copy(SQ.at[n], RQ.at[n], s_gq.at[n], r_gq.at[n], **where)

    def query_send(k):
        swap(k).wait_recv()
        for n, (kk, d, e) in enumerate(legs):
            if kk == k:
                x_ = query_sum(k, d)
                for m in {2: {0: (0, 2), 1: (3,)}, 6: {0: (4,), 1: (1, 5)}}.get(k, {}).get(d, ()):
                    leg(m).wait_recv()
                    x_ = x_ + take(RQ.at[m])
                put(SQ.at[n], x_)
                start(leg(n))

    split = (pl.ds(0, FIRST), pl.ds(FIRST, ROWS - FIRST))
    own, sp, rp, sp2, rp2 = (OWN1, OWN2), (SP1, SP2), (RP1, RP2), (SS1, SS2), (RS1, RS2)

    def plane_leg(half, e, t):
        at = (half, e - 1, t)
        return copy(sp[half].at[e - 1, t], rp[half].at[e - 1, t], s_gp.at[at], r_gp.at[at], **along(half, e))

    def plane_last(half, t):
        at = (half, 3, t)
        return copy(sp2[half].at[t - 1], rp2[half].at[t - 1], s_gp.at[at], r_gp.at[at], **along(1 - half, t))

    def passage_product(a, b):
        tx, ty = lax.rem(x + a, NX), lax.rem(y + b, NY)
        cols = pl.ds(pl.multiple_of((ty * 2 + lax.rem(tx, 2)) * 128, 128), 128)
        part = tn(W[:, cols], Q[tx // 2].reshape(TILE, WIDE))
        for half, e, t in ((0, a, b), (1, b, a)):
            rows = part[0:FIRST] if half == 0 else part[FIRST:]
            if e:
                put(sp[half].at[e - 1, t], rows)
                start(plane_leg(half, e, t))
            else:
                own[half][t] = rows

    def plane_sum(half, t):
        total = own[half][t]
        for e in (1, 3, 2):
            plane_leg(half, e, t).wait_recv()
            total = total + take(rp[half].at[e - 1, t])
        return total

    def plane_send(t):
        for half in range(2):
            put(sp2[half].at[t - 1], plane_sum(half, t))
            start(plane_last(half, t))

    for k in (4, 3, 5):
        query_product(k)
    for a, b in ((2, 2), (1, 2), (2, 1)):
        passage_product(a, b)
    for k in (4, 3, 5):
        query_send(k)
    for a, b in ((3, 2), (2, 3), (0, 2), (2, 0)):
        passage_product(a, b)
    for k in (2, 6, 1, 7, 0):
        query_product(k)
    for a, b in ((1, 1), (3, 1), (1, 3), (3, 3)):
        passage_product(a, b)
    for k in (1, 7, 0):
        query_send(k)
    for a, b in ((0, 1), (1, 0), (0, 3), (3, 0), (0, 0)):
        passage_product(a, b)
    plane_send(2)
    for k in (2, 6):
        query_send(k)
    plane_send(1)
    plane_send(3)
    for half in range(2):
        total = plane_sum(half, 0)
        for t in (2, 1, 3):
            plane_last(half, t).wait_recv()
            total = total + take(rp2[half].at[t - 1])
        gp_ref[split[half], :] = total * factor
    total = query_sum(0, 0)
    for n in (10, 12, 6, 8):
        leg(n).wait_recv()
        total = total + take(RQ.at[n])
    gq_ref[own_rows, :] = total * factor
    total = jnp.zeros((HALF, WIDE), jnp.float32)
    for n in (14, 11, 13, 7, 9):
        leg(n).wait_recv()
        total = total + take(RQ.at[n])
    gq_ref[other_rows, :] = total * factor
    for cp in sends:
        cp.wait_send()


def local(queries, passages, positives):
    dma = pltpu.SemaphoreType.DMA
    vmem = pl.BlockSpec(memory_space=pltpu.VMEM)
    out = jax.ShapeDtypeStruct((ROWS, WIDE), jnp.float32)
    parts = (FIRST, ROWS - FIRST)
    bf16, f32, i16 = jnp.bfloat16, jnp.float32, jnp.int16
    return pl.pallas_call(
        kernel,
        out_shape=(out, out),
        in_specs=[vmem] * 3,
        out_specs=(vmem, vmem),
        scratch_shapes=[
            pltpu.VMEM((2, 16, HALF, WIDE), bf16),
            pltpu.VMEM((2, 8, ROWS, WIDE), bf16),
            pltpu.VMEM((TILE, TILE), f32),
            pltpu.VMEM((TILE, TILE), bf16),
            pltpu.VMEM((TILE, 128), jnp.int32),
            pltpu.VMEM((128, 128), jnp.int32),
            pltpu.VMEM((8, TILE), f32),
            pltpu.VMEM((8, TILE), f32),
            pltpu.VMEM((16, 8, 128), f32),
            pltpu.VMEM((16, 8, 128), f32),
            pltpu.VMEM((8, 128), f32),
            pltpu.VMEM((8, 128), f32),
            pltpu.VMEM((8, 128), f32),
            pltpu.VMEM((8, 2, HALF, WIDE), f32),
            pltpu.VMEM((8, 2, 2, HALF, WIDE), f32),
            pltpu.VMEM((15, 2 * HALF + 16, 128), i16),
            pltpu.VMEM((15, 2 * HALF + 16, 128), i16),
            *(pltpu.VMEM((4, r, WIDE), f32) for r in parts),
            *(pltpu.VMEM((3, 4, 2 * r + 16, 128), i16) for _ in range(2) for r in parts),
            *(pltpu.VMEM((3, 2 * r + 16, 128), i16) for _ in range(2) for r in parts),
            dma, dma,
            dma((2, 5, 4)), dma((2, 5, 4)),
            dma((2, 8)), dma((2, 8)),
            dma((8, 2)), dma((8, 2)),
            dma((16,)), dma((16,)),
            dma((16,)), dma((16,)),
            dma((8,)), dma((8,)),
            dma((2, 4, 4)), dma((2, 4, 4)),
            dma((15,)), dma((15,)),
        ],
        compiler_params=pltpu.CompilerParams(
            collective_id=0, has_side_effects=True, vmem_limit_bytes=60 * 1024 * 1024
        ),
    )(queries, passages, positives.reshape(128, 128))


def solution(mesh):
    split = Mesh(
        mesh.devices.reshape(NZ, NY, 2, 2, mesh.shape["rep"]),
        AXES,
    )
    return jax.shard_map(
        local,
        mesh=split,
        in_specs=(P(BATCH, "xh"), P(BATCH, "xh"), P()),
        out_specs=(P(BATCH, "xh"), P(BATCH, "xh")),
        check_vma=False,
    )
```

```python
import math

import jax
import jax.numpy as jnp
from jax import lax
from jax.experimental import pallas as pl
from jax.experimental.pallas import tpu as pltpu
from jax.sharding import Mesh
from jax.sharding import PartitionSpec as P

AXES = ("z", "y", "xl", "c", "xh")
BATCH = ("z", "y", "xl", "c")
NX, NY, NZ = 4, 4, 8
MESH = pl.DeviceIdType.MESH
ROWS = 128
HALF = 64
WIDE = 256
TILE = 1024
FIRST = 64
STEP = 32000.0
LOG2E = 1.4426950408889634
LN2 = 0.6931471805599453


def put(ref, x):
    rows = x.shape[0]
    top = jnp.max(jnp.abs(x), axis=0, keepdims=True)
    power = jnp.clip(jnp.floor(jnp.log(top) * LOG2E) + 1.0, -120.0, 120.0)
    value = jnp.round(x * (STEP * jnp.exp2(-power))).astype(jnp.int32).astype(jnp.int16)
    ref[0:rows] = value[:, :128]
    ref[rows : 2 * rows] = value[:, 128:]
    both = [jnp.broadcast_to(power[:, at : at + 128], (8, 128)) for at in (0, 128)]
    ref[2 * rows :] = jnp.concatenate(both, axis=0).astype(jnp.int32).astype(jnp.int16)


def take(ref):
    rows = (ref.shape[0] - 16) // 2
    unit = jnp.exp2(ref[2 * rows :].astype(jnp.int32).astype(jnp.float32)) * (1.0 / STEP)
    value = ref[0 : 2 * rows].astype(jnp.int32).astype(jnp.float32)
    return jnp.concatenate([value[:rows] * unit[0:1], value[rows:] * unit[8:9]], axis=1)


def to_lanes(column):
    return jnp.broadcast_to(column, (128, 128)).T[:1]


def to_rows(line):
    return jnp.broadcast_to(line, (128, 128)).T


def join(stack):
    high = jnp.max(stack, axis=0)
    return high + jnp.log(jnp.sum(jnp.exp2(stack - high[None]), axis=0)) * LOG2E


def nt(a, b):
    return lax.dot_general(a, b, (((1,), (1,)), ((), ())), preferred_element_type=jnp.float32)


def tn(a, b):
    return lax.dot_general(a, b, (((0,), (0,)), ((), ())), preferred_element_type=jnp.float32)


def kernel(
    q_hbm, p_hbm, pos_hbm, gq_ref, gp_ref, q_ref, p_ref, pos_ref,
    Q, PT, S, W, posc, tmp, cmax, csum, rstat, cstat, rown, cown, rfin,
    XQ, GQ, SQ, RQ, OWN1, OWN2, SP1, SP2, RP1, RP2, SS1, SS2, RS1, RS2,
    s_in, s_xq, r_xq, s_p, r_p, s_q, r_q, s_d, r_d, s_rs, r_rs, s_cs, r_cs,
    s_x, r_x, s_gp, r_gp, s_gq, r_gq,
):
    z, y, xl, c, xh = (lax.axis_index(a) for a in AXES)
    x = xh * 2 + xl
    factor = 1.0 / math.sqrt(2 * WIDE)

    def copy(src, dst, ssem, rsem, **where):
        return pltpu.make_async_remote_copy(
            src_ref=src, dst_ref=dst, send_sem=ssem, recv_sem=rsem,
            device_id=where, device_id_type=MESH,
        )

    def plane(k):
        tx, ty = lax.rem(x + k % 4, NX), lax.rem(y + k // 4, NY)
        return tx, ty, {"xh": tx // 2, "xl": lax.rem(tx, 2), "y": ty}

    def pillar(k):
        tz, tc = lax.rem(z + k // 2, NZ), lax.rem(c + k % 2, 2)
        return tz, tc, {"z": tz, "c": tc}

    def along(axis, e):
        if axis == 0:
            t = lax.rem(x + e, NX)
            return {"xh": t // 2, "xl": lax.rem(t, 2)}
        return {"y": lax.rem(y + e, NY)} if axis == 1 else {"z": lax.rem(z + e, NZ)}

    barrier = pltpu.get_barrier_semaphore()
    near = [along(axis, e) for e in (1, 2, 3) for axis in (0, 1)]
    near += [along(2, e) for e in (1, 7, 2, 6)] + [{"c": 1 - c}]
    for where in near:
        pl.semaphore_signal(barrier, inc=1, device_id=where, device_id_type=MESH)
    loads = [
        pltpu.make_async_copy(src, dst, s_in.at[n])
        for n, (src, dst) in enumerate(((q_hbm, q_ref), (p_hbm, p_ref), (pos_hbm, pos_ref)))
    ]
    for load in loads:
        load.start()
    for load in loads:
        load.wait()
    pl.semaphore_wait(barrier, len(near))

    slot_q = z * 2 + c
    slot_p = y * 2 + xl
    own_rows = pl.ds(pl.multiple_of(xh * HALF, HALF), HALF)
    other_rows = pl.ds(pl.multiple_of((1 - xh) * HALF, HALF), HALF)
    sends = []

    def start(cp):
        cp.start()
        sends.append(cp)

    def plane_copy(half, phase, e, f, sender):
        first, second = (0, 1) if half == 0 else (1, 0)
        off = [0, 0]
        if phase:
            off[first] -= f
        if not sender:
            off[second if phase else first] -= e
        ox, oy = lax.rem(x + off[0] % 4, NX), lax.rem(y + off[1] % 4, NY)
        rows = pl.ds(half * HALF, HALF)
        dst = PT.at[ox // 2, oy * 2 + lax.rem(ox, 2), rows]
        src = p_ref.at[rows] if sender and f == 0 else dst
        at = (half, phase * (f + 1), e)
        return copy(src, dst, s_p.at[at], r_p.at[at], **along(second if phase else first, e))

    def ring_copy(group, hop, back, e, rows, number, sender):
        oz = lax.rem(z + (16 - back - (0 if sender else e)) % NZ, NZ)
        h = xh if group == 0 else 1 - xh
        dst = Q.at[h, oz * 2 + c, rows]
        src = dst
        if sender and back == 0 and group == 0:
            src = q_ref.at[own_rows]
        at = (group, number)
        return copy(src, dst, s_q.at[at], r_q.at[at], **along(2, e % NZ))

    whole, low, high = pl.ds(0, HALF), pl.ds(0, 32), pl.ds(32, 32)
    hops = [(0, 0, 2, whole), (0, 0, -2, whole), (0, 0, 1, whole), (0, 0, -1, whole),
            (1, 2, 2, low), (1, -2, -2, high), (1, 2, 1, whole), (1, -2, -1, whole)]

    def ring(group, n, sender):
        return ring_copy(group, *hops[n], n, sender)

    def across(k, group, source):
        h = xh if group == 0 else 1 - xh
        oz = lax.rem(z + k, NZ)
        dst = Q.at[h, oz * 2 + (c if source else 1 - c)]
        src = q_ref.at[own_rows] if source and isinstance(k, int) and k == 0 and group == 0 else Q.at[h, oz * 2 + c]
        return copy(src, dst, s_d.at[k, group], r_d.at[k, group], c=1 - c)

    def ring_take(group, n, *ks):
        for m in n:
            ring(group, m, False).wait_recv()
        for k in ks:
            start(across(k, group, True))

    start(copy(q_ref.at[other_rows], Q.at[xh, slot_q], s_xq, r_xq, **along(0, 2)))
    for e in (2, 1, 3):
        for half in range(2):
            start(plane_copy(half, 0, e, 0, True))
    for n in range(4):
        start(ring(0, n, True))
    for e in (2, 1, 3):
        for half in range(2):
            start(plane_copy(half, 1, e, 0, True))
    start(across(0, 0, True))
    Q[xh, slot_q] = q_ref[own_rows, :]
    PT[xh, slot_p] = p_ref[...]

    for s in range(16):
        line = (s // 2) * 16 + y * 4 + xl * 2 + s % 2
        tmp[...] = to_rows(pos_ref[pl.ds(line, 1), :])
        posc[s * HALF : (s + 1) * HALF] = tmp[own_rows, :]

    def plane_pass(f):
        for half in range(2):
            plane_copy(half, 0, f, 0, False).wait_recv()
            for e in (2, 1, 3):
                start(plane_copy(half, 1, e, f, True))

    plane_pass(1)
    plane_pass(3)
    copy(q_ref.at[own_rows], Q.at[1 - xh, slot_q], s_xq, r_xq, **along(0, 2)).wait_recv()
    for n in range(4):
        start(ring(1, n, True))
    start(across(0, 1, True))
    plane_pass(2)
    ring_take(0, (0,), 6)
    start(ring(0, 4, True))
    start(ring(0, 6, True))
    ring_take(0, (1,), 2)
    start(ring(0, 5, True))
    start(ring(0, 7, True))
    ring_take(0, (2,), 7)
    ring_take(0, (3,), 1)
    ring_take(1, (0,), 6)
    start(ring(1, 4, True))
    start(ring(1, 6, True))
    ring_take(1, (1,), 2)
    start(ring(1, 5, True))
    start(ring(1, 7, True))
    ring_take(1, (2,), 7)
    ring_take(1, (3,), 1)
    for half in range(2):
        for f in range(4):
            for e in (1, 2, 3):
                plane_copy(half, 1, e, f, False).wait_recv()
    ring_take(0, (6,), 5)
    ring_take(0, (7,), 3)
    ring_take(0, (4, 5), 4)

    def score(n, carry):
        k = lax.rem(lax.select(lax.rem(n, 2) == 1, (n + 1) // 2, NZ - n // 2), NZ)
        i = lax.rem(z + k, NZ)
        for group in range(2):
            across(k, group, False).wait_recv()
        rows = pl.ds(pl.multiple_of(i * 128, 128), 128)
        part = [
            nt(Q[h, pl.ds(i * 2, 2)].reshape(128, WIDE), PT[h].reshape(TILE, WIDE))
            for h in range(2)
        ]
        s = (part[0] + part[1]) * (factor * LOG2E)
        S[rows] = s
        high = jnp.max(s, axis=1, keepdims=True)
        total = jnp.sum(jnp.exp2(s - high), axis=1, keepdims=True)
        rown[pl.ds(i, 1)] = to_lanes(high + jnp.log(total) * LOG2E)
        chigh = jnp.max(s, axis=0, keepdims=True)
        cmax[pl.ds(n, 1)] = chigh
        csum[pl.ds(n, 1)] = jnp.sum(jnp.exp2(s - chigh), axis=0, keepdims=True)
        return carry

    lax.fori_loop(0, 3, score, 0)
    ring_take(1, (6,), 5)
    ring_take(1, (7,), 3)
    ring_take(1, (4, 5), 4)
    lax.fori_loop(3, 8, score, 0)
    chigh = jnp.max(cmax[...], axis=0, keepdims=True)
    ctotal = jnp.sum(csum[...] * jnp.exp2(cmax[...] - chigh), axis=0, keepdims=True)
    cnorm = chigh + jnp.log(ctotal) * LOG2E
    for b in range(8):
        cown[b : b + 1] = cnorm[:, b * 128 : (b + 1) * 128]
    rstat[0] = rown[...]
    cstat[0] = cown[...]
    for k in range(1, 16):
        cp = copy(rown, rstat.at[k], s_rs.at[k], r_rs.at[k], **pillar(k)[2])
        cp.start()
        sends.append(cp)
        cp = copy(cown, cstat.at[k], s_cs.at[k], r_cs.at[k], **plane(k)[2])
        cp.start()
        sends.append(cp)
    for k in range(1, 16):
        copy(rown, rstat.at[k], s_rs.at[k], r_rs.at[k], **pillar(k)[2]).wait_recv()
        copy(cown, cstat.at[k], s_cs.at[k], r_cs.at[k], **plane(k)[2]).wait_recv()
    rown2 = join(rstat[...])
    cown2 = join(cstat[...])
    cmax[0:1] = jnp.concatenate([cown2[b : b + 1] for b in range(8)], axis=1)
    rfin[...] = rown2

    def weigh(i, carry):
        rows = pl.ds(pl.multiple_of(i * 128, 128), 128)
        rnorm = to_rows(rfin[pl.ds(i, 1), :])
        for b in range(8):
            cols = slice(b * 128, (b + 1) * 128)
            s = S[rows, cols]
            first = ((z * 4 + b // 2) * 2 + b % 2) * 2 + c
            ids = first * ROWS + lax.broadcasted_iota(jnp.int32, (128, 128), 1)
            match = jnp.where(posc[rows, :] == ids, 2.0, 0.0)
            w = jnp.exp2(s - rnorm) + jnp.exp2(s - cmax[0:1, cols]) - match
            W[rows, cols] = w.astype(jnp.bfloat16)
        return carry

    lax.fori_loop(0, 8, weigh, 0)

    def query_product(k):
        rows = pl.ds(pl.multiple_of(lax.rem(z + k, NZ) * 128, 128), 128)
        for h in range(2):
            part = jnp.dot(W[rows, :], PT[h].reshape(TILE, WIDE), preferred_element_type=jnp.float32)
            part = part.reshape(2, HALF, WIDE)
            GQ[k, 0, h] = part[0]
            GQ[k, 1, h] = part[1]
        start(swap(k))

    def swap(k):
        return copy(GQ.at[k, 1 - c], XQ.at[k], s_x.at[k], r_x.at[k], c=1 - c)

    def side(d):
        return xh if d == 0 else 1 - xh

    def query_sum(k, d):
        return GQ[k, c, side(d)] + XQ[k, side(d)]

    legs = [(4, 0, 2), (4, 1, -2), (3, 0, 1), (3, 1, 1), (5, 0, -1), (5, 1, -1),
            (2, 0, 2), (2, 1, 2), (6, 0, -2), (6, 1, -2), (1, 0, 1), (1, 1, 1), (7, 0, -1), (7, 1, -1), (0, 1, 0)]

    def leg(n):
        k, d, e = legs[n]
        where = along(2, e % NZ) if e else {}
        if n >= 6 and d:
            where["xh"] = 1 - xh
        return copy(SQ.at[n], RQ.at[n], s_gq.at[n], r_gq.at[n], **where)

    def query_send(k):
        swap(k).wait_recv()
        for n, (kk, d, e) in enumerate(legs):
            if kk == k:
                x_ = query_sum(k, d)
                for m in {2: {0: (0, 2), 1: (3,)}, 6: {0: (4,), 1: (1, 5)}}.get(k, {}).get(d, ()):
                    leg(m).wait_recv()
                    x_ = x_ + take(RQ.at[m])
                put(SQ.at[n], x_)
                start(leg(n))

    split = (pl.ds(0, FIRST), pl.ds(FIRST, ROWS - FIRST))
    own, sp, rp, sp2, rp2 = (OWN1, OWN2), (SP1, SP2), (RP1, RP2), (SS1, SS2), (RS1, RS2)

    def plane_leg(half, e, t):
        at = (half, e - 1, t)
        return copy(sp[half].at[e - 1, t], rp[half].at[e - 1, t], s_gp.at[at], r_gp.at[at], **along(half, e))

    def plane_last(half, t):
        at = (half, 3, t)
        return copy(sp2[half].at[t - 1], rp2[half].at[t - 1], s_gp.at[at], r_gp.at[at], **along(1 - half, t))

    def passage_product(a, b):
        tx, ty = lax.rem(x + a, NX), lax.rem(y + b, NY)
        cols = pl.ds(pl.multiple_of((ty * 2 + lax.rem(tx, 2)) * 128, 128), 128)
        part = tn(W[:, cols], Q[tx // 2].reshape(TILE, WIDE))
        for half, e, t in ((0, a, b), (1, b, a)):
            rows = part[0:FIRST] if half == 0 else part[FIRST:]
            if e:
                put(sp[half].at[e - 1, t], rows)
                start(plane_leg(half, e, t))
            else:
                own[half][t] = rows

    def plane_sum(half, t):
        total = own[half][t]
        for e in (1, 3, 2):
            plane_leg(half, e, t).wait_recv()
            total = total + take(rp[half].at[e - 1, t])
        return total

    def plane_send(t):
        for half in range(2):
            put(sp2[half].at[t - 1], plane_sum(half, t))
            start(plane_last(half, t))

    for k in (4, 3, 5,):
        query_product(k)
    for a, b in ((2, 2), (1, 2), (2, 1),):
        passage_product(a, b)
    for k in (4, 3, 5,):
        query_send(k)
    for a, b in ((3, 2), (2, 3), (0, 2), (2, 0),):
        passage_product(a, b)
    for k in (2, 6, 1, 7, 0,):
        query_product(k)
    for a, b in ((1, 1), (3, 1), (1, 3), (3, 3),):
        passage_product(a, b)
    for k in (1, 7, 0,):
        query_send(k)
    for a, b in ((0, 1), (1, 0), (0, 3), (3, 0), (0, 0),):
        passage_product(a, b)
    for k in (2, 6,):
        query_send(k)
    for k in (2, 1, 3,):
        plane_send(k)
    for half in range(2):
        total = plane_sum(half, 0)
        for t in (2, 1, 3):
            plane_last(half, t).wait_recv()
            total = total + take(rp2[half].at[t - 1])
        gp_ref[split[half], :] = total * factor
    total = query_sum(0, 0)
    for n in (10, 12, 6, 8):
        leg(n).wait_recv()
        total = total + take(RQ.at[n])
    gq_ref[own_rows, :] = total * factor
    total = jnp.zeros((HALF, WIDE), jnp.float32)
    for n in (14, 11, 13, 7, 9):
        leg(n).wait_recv()
        total = total + take(RQ.at[n])
    gq_ref[other_rows, :] = total * factor
    for cp in sends:
        cp.wait_send()


def local(queries, passages, positives):
    dma = pltpu.SemaphoreType.DMA
    vmem = pl.BlockSpec(memory_space=pltpu.VMEM)
    out = pltpu.VMEM((ROWS, WIDE), jnp.float32)
    parts = (FIRST, ROWS - FIRST)
    bf16, f32, i16 = jnp.bfloat16, jnp.float32, jnp.int16
    return pl.pallas_call(
        kernel,
        out_shape=(out, out),
        in_specs=[pl.BlockSpec(memory_space=pl.ANY)] * 3,
        out_specs=(vmem, vmem),
        scratch_shapes=[
            *(pltpu.VMEM((ROWS, WIDE), bf16) for _ in range(2)),
            pltpu.VMEM((128, 128), jnp.int32),
            pltpu.VMEM((2, 16, HALF, WIDE), bf16),
            pltpu.VMEM((2, 8, ROWS, WIDE), bf16),
            pltpu.VMEM((TILE, TILE), f32),
            pltpu.VMEM((TILE, TILE), bf16),
            pltpu.VMEM((TILE, 128), jnp.int32),
            pltpu.VMEM((128, 128), jnp.int32),
            pltpu.VMEM((8, TILE), f32),
            pltpu.VMEM((8, TILE), f32),
            pltpu.VMEM((16, 8, 128), f32),
            pltpu.VMEM((16, 8, 128), f32),
            pltpu.VMEM((8, 128), f32),
            pltpu.VMEM((8, 128), f32),
            pltpu.VMEM((8, 128), f32),
            pltpu.VMEM((8, 2, HALF, WIDE), f32),
            pltpu.VMEM((8, 2, 2, HALF, WIDE), f32),
            pltpu.VMEM((15, 2 * HALF + 16, 128), i16),
            pltpu.VMEM((15, 2 * HALF + 16, 128), i16),
            *(pltpu.VMEM((4, r, WIDE), f32) for r in parts),
            *(pltpu.VMEM((3, 4, 2 * r + 16, 128), i16) for _ in range(2) for r in parts),
            *(pltpu.VMEM((3, 2 * r + 16, 128), i16) for _ in range(2) for r in parts),
            dma((3,)),
            dma, dma,
            dma((2, 5, 4)), dma((2, 5, 4)),
            dma((2, 8)), dma((2, 8)),
            dma((8, 2)), dma((8, 2)),
            dma((16,)), dma((16,)),
            dma((16,)), dma((16,)),
            dma((8,)), dma((8,)),
            dma((2, 4, 4)), dma((2, 4, 4)),
            dma((15,)), dma((15,)),
        ],
        compiler_params=pltpu.CompilerParams(
            collective_id=0, has_side_effects=True, vmem_limit_bytes=60 * 1024 * 1024
        ),
    )(queries, passages, positives.reshape(128, 128))


def solution(mesh):
    split = Mesh(
        mesh.devices.reshape(NZ, NY, 2, 2, mesh.shape["rep"]),
        AXES,
    )
    return jax.shard_map(
        local,
        mesh=split,
        in_specs=(P(BATCH, "xh"), P(BATCH, "xh"), P()),
        out_specs=(P(BATCH, "xh"), P(BATCH, "xh")),
        check_vma=False,
    )
```

```python
import math

import jax
import jax.numpy as jnp
from jax import lax
from jax.experimental import pallas as pl
from jax.experimental.pallas import tpu as pltpu
from jax.sharding import Mesh
from jax.sharding import PartitionSpec as P

AXES = ("z", "y", "xl", "c", "xh")
BATCH = ("z", "y", "xl", "c")
NX, NY, NZ = 4, 4, 8
MESH = pl.DeviceIdType.MESH
ROWS = 128
HALF = 64
WIDE = 256
TILE = 1024
ORDER = (0, 1, 7, 2, 6, 3, 5, 4)
POS = tuple(ORDER.index(k) for k in range(8))
SPLIT = 4
FIRST = 64
STEP = 32000.0
LOG2E = 1.4426950408889634
LN2 = 0.6931471805599453


def put(ref, x):
    rows = x.shape[0]
    top = jnp.max(jnp.abs(x), axis=0, keepdims=True)
    power = jnp.clip(jnp.floor(jnp.log(top) * LOG2E) + 1.0, -120.0, 120.0)
    value = jnp.round(x * (STEP * jnp.exp2(-power))).astype(jnp.int32).astype(jnp.int16)
    ref[0:rows] = value[:, :128]
    ref[rows : 2 * rows] = value[:, 128:]
    both = [jnp.broadcast_to(power[:, at : at + 128], (8, 128)) for at in (0, 128)]
    ref[2 * rows :] = jnp.concatenate(both, axis=0).astype(jnp.int32).astype(jnp.int16)


def take(ref):
    rows = (ref.shape[0] - 16) // 2
    unit = jnp.exp2(ref[2 * rows :].astype(jnp.int32).astype(jnp.float32)) * (1.0 / STEP)
    value = ref[0 : 2 * rows].astype(jnp.int32).astype(jnp.float32)
    return jnp.concatenate([value[:rows] * unit[0:1], value[rows:] * unit[8:9]], axis=1)


def to_lanes(column):
    return jnp.broadcast_to(column, (128, 128)).T[:1]


def to_rows(line):
    return jnp.broadcast_to(line, (128, 128)).T


def join(stack):
    high = jnp.max(stack, axis=0)
    return high + jnp.log(jnp.sum(jnp.exp2(stack - high[None]), axis=0)) * LOG2E


def nt(a, b):
    return lax.dot_general(a, b, (((1,), (1,)), ((), ())), preferred_element_type=jnp.float32)


def tn(a, b):
    return lax.dot_general(a, b, (((0,), (0,)), ((), ())), preferred_element_type=jnp.float32)


def kernel(
    q_hbm, p_hbm, pos_hbm, gq_ref, gp_ref, q_ref, p_ref, pos_ref,
    Q, PT, S, W, posc, tmp, cmax, csum, rstat, cstat, rown, cown, rfin,
    XQ, GQ, SQ, RQ, OWN1, OWN2, SP1, SP2, RP1, RP2, SS1, SS2, RS1, RS2,
    s_in, s_xq, r_xq, s_p, r_p, s_q, r_q, s_d, r_d, s_rs, r_rs, s_cs, r_cs,
    s_x, r_x, s_gp, r_gp, s_gq, r_gq,
):
    z, y, xl, c, xh = (lax.axis_index(a) for a in AXES)
    x = xh * 2 + xl
    factor = 1.0 / math.sqrt(2 * WIDE)

    def copy(src, dst, ssem, rsem, **where):
        return pltpu.make_async_remote_copy(
            src_ref=src, dst_ref=dst, send_sem=ssem, recv_sem=rsem,
            device_id=where, device_id_type=MESH,
        )

    def plane(k):
        tx, ty = lax.rem(x + k % 4, NX), lax.rem(y + k // 4, NY)
        return tx, ty, {"xh": tx // 2, "xl": lax.rem(tx, 2), "y": ty}

    def pillar(k):
        tz, tc = lax.rem(z + k // 2, NZ), lax.rem(c + k % 2, 2)
        return tz, tc, {"z": tz, "c": tc}

    def along(axis, e):
        if axis == 0:
            t = lax.rem(x + e, NX)
            return {"xh": t // 2, "xl": lax.rem(t, 2)}
        return {"y": lax.rem(y + e, NY)} if axis == 1 else {"z": lax.rem(z + e, NZ)}

    barrier = pltpu.get_barrier_semaphore()
    near = [along(axis, e) for e in (1, 2, 3) for axis in (0, 1)]
    near += [along(2, e) for e in (1, 7, 2, 6)] + [{"c": 1 - c}]
    for where in near:
        pl.semaphore_signal(barrier, inc=1, device_id=where, device_id_type=MESH)
    loads = [
        pltpu.make_async_copy(src, dst, s_in.at[n])
        for n, (src, dst) in enumerate(((q_hbm, q_ref), (p_hbm, p_ref), (pos_hbm, pos_ref)))
    ]
    for load in loads:
        load.start()
    for load in loads:
        load.wait()
    pl.semaphore_wait(barrier, len(near))

    slot_p = y * 2 + xl
    own_rows = pl.ds(pl.multiple_of(xh * HALF, HALF), HALF)
    other_rows = pl.ds(pl.multiple_of((1 - xh) * HALF, HALF), HALF)
    sends = []

    def start(cp):
        cp.start()
        sends.append(cp)

    def plane_copy(half, phase, e, f, sender):
        first, second = (0, 1) if half == 0 else (1, 0)
        off = [0, 0]
        if phase:
            off[first] -= f
        if not sender:
            off[second if phase else first] -= e
        ox, oy = lax.rem(x + off[0] % 4, NX), lax.rem(y + off[1] % 4, NY)
        rows = pl.ds(half * HALF, HALF)
        dst = PT.at[ox // 2, oy * 2 + lax.rem(ox, 2), rows]
        src = p_ref.at[rows] if sender and f == 0 else dst
        at = (half, phase * (f + 1), e)
        return copy(src, dst, s_p.at[at], r_p.at[at], **along(second if phase else first, e))

    def ring_copy(group, hop, back, e, rows, number, sender):
        h = xh if group == 0 else 1 - xh
        src = Q.at[h, POS[-back % NZ], c, rows]
        dst = Q.at[h, POS[(-back - e) % NZ], c, rows]
        if sender and back == 0 and group == 0:
            src = q_ref.at[own_rows]
        at = (group, number)
        return copy(src, dst, s_q.at[at], r_q.at[at], **along(2, e % NZ))

    whole, low, high = pl.ds(0, HALF), pl.ds(0, 32), pl.ds(32, 32)
    hops = [(0, 0, 2, whole), (0, 0, -2, whole), (0, 0, 1, whole), (0, 0, -1, whole),
            (1, 2, 2, low), (1, -2, -2, high), (1, 2, 1, whole), (1, -2, -1, whole)]

    def ring(group, n, sender):
        return ring_copy(group, *hops[n], n, sender)

    def across(k, group, source):
        h = xh if group == 0 else 1 - xh
        src = q_ref.at[own_rows] if k == 0 and group == 0 else Q.at[h, POS[k], c]
        dst = Q.at[h, POS[k], c if source else 1 - c]
        return copy(src, dst, s_d.at[k, group], r_d.at[k, group], c=1 - c)

    def ring_take(group, n, *ks):
        for m in n:
            ring(group, m, False).wait_recv()
        for k in ks:
            start(across(k, group, True))

    start(copy(q_ref.at[other_rows], Q.at[xh, 0, c], s_xq, r_xq, **along(0, 2)))
    for e in (2, 1, 3):
        for half in range(2):
            start(plane_copy(half, 0, e, 0, True))
    for n in range(4):
        start(ring(0, n, True))
    for e in (2, 1, 3):
        for half in range(2):
            start(plane_copy(half, 1, e, 0, True))
    start(across(0, 0, True))
    Q[xh, 0, c] = q_ref[own_rows, :]
    PT[xh, slot_p] = p_ref[...]

    for s in range(16):
        line = lax.rem(z + ORDER[s // 2], NZ) * 16 + y * 4 + xl * 2 + s % 2
        tmp[...] = to_rows(pos_ref[pl.ds(line, 1), :])
        posc[s * HALF : (s + 1) * HALF] = tmp[own_rows, :]

    def plane_pass(f):
        for half in range(2):
            plane_copy(half, 0, f, 0, False).wait_recv()
            for e in (2, 1, 3):
                start(plane_copy(half, 1, e, f, True))

    plane_pass(1)
    plane_pass(3)
    copy(q_ref.at[own_rows], Q.at[1 - xh, 0, c], s_xq, r_xq, **along(0, 2)).wait_recv()
    for n in range(4):
        start(ring(1, n, True))
    start(across(0, 1, True))
    plane_pass(2)
    ring_take(0, (0,), 6)
    start(ring(0, 4, True))
    start(ring(0, 6, True))
    ring_take(0, (1,), 2)
    start(ring(0, 5, True))
    start(ring(0, 7, True))
    ring_take(0, (2,), 7)
    ring_take(0, (3,), 1)
    ring_take(1, (0,), 6)
    start(ring(1, 4, True))
    start(ring(1, 6, True))
    ring_take(1, (1,), 2)
    start(ring(1, 5, True))
    start(ring(1, 7, True))
    ring_take(1, (2,), 7)
    ring_take(1, (3,), 1)
    for half in range(2):
        for f in range(4):
            for e in (1, 2, 3):
                plane_copy(half, 1, e, f, False).wait_recv()
    ring_take(0, (6,), 5)
    ring_take(0, (7,), 3)
    ring_take(0, (4, 5), 4)

    def tile_z(n):
        odd = lax.rem(n, 2) == 1
        k = jnp.where(odd, (n + 1) // 2, NZ - n // 2)
        return lax.rem(z + k, NZ)

    def score_dots(first, last):
        for n in range(first, last):
            for group in range(2):
                across(ORDER[n], group, False).wait_recv()
        part = [
            nt(Q[h, first:last].reshape((last - first) * 128, WIDE), PT[h].reshape(TILE, WIDE))
            for h in range(2)
        ]
        S[first * 128 : last * 128] = (part[0] + part[1]) * (factor * LOG2E)

    def score(n, carry):
        s = S[pl.ds(pl.multiple_of(n * 128, 128), 128)]
        high = jnp.max(s, axis=1, keepdims=True)
        total = jnp.sum(jnp.exp2(s - high), axis=1, keepdims=True)
        rown[pl.ds(tile_z(n), 1)] = to_lanes(high + jnp.log(total) * LOG2E)
        chigh = jnp.max(s, axis=0, keepdims=True)
        cmax[pl.ds(n, 1)] = chigh
        csum[pl.ds(n, 1)] = jnp.sum(jnp.exp2(s - chigh), axis=0, keepdims=True)
        return carry

    score_dots(0, SPLIT)
    lax.fori_loop(0, SPLIT, score, 0)
    ring_take(1, (6,), 5)
    ring_take(1, (7,), 3)
    ring_take(1, (4, 5), 4)
    score_dots(SPLIT, 8)
    lax.fori_loop(SPLIT, 8, score, 0)
    chigh = jnp.max(cmax[...], axis=0, keepdims=True)
    ctotal = jnp.sum(csum[...] * jnp.exp2(cmax[...] - chigh), axis=0, keepdims=True)
    cnorm = chigh + jnp.log(ctotal) * LOG2E
    for b in range(8):
        cown[b : b + 1] = cnorm[:, b * 128 : (b + 1) * 128]
    rstat[0] = rown[...]
    cstat[0] = cown[...]
    for k in range(1, 16):
        cp = copy(rown, rstat.at[k], s_rs.at[k], r_rs.at[k], **pillar(k)[2])
        cp.start()
        sends.append(cp)
        cp = copy(cown, cstat.at[k], s_cs.at[k], r_cs.at[k], **plane(k)[2])
        cp.start()
        sends.append(cp)
    for k in range(1, 16):
        copy(rown, rstat.at[k], s_rs.at[k], r_rs.at[k], **pillar(k)[2]).wait_recv()
        copy(cown, cstat.at[k], s_cs.at[k], r_cs.at[k], **plane(k)[2]).wait_recv()
    rown2 = join(rstat[...])
    cown2 = join(cstat[...])
    cmax[0:1] = jnp.concatenate([cown2[b : b + 1] for b in range(8)], axis=1)
    rfin[...] = rown2

    def weigh(i, carry):
        rows = pl.ds(pl.multiple_of(i * 128, 128), 128)
        rnorm = to_rows(rfin[pl.ds(tile_z(i), 1), :])
        for b in range(8):
            cols = slice(b * 128, (b + 1) * 128)
            s = S[rows, cols]
            first = ((z * 4 + b // 2) * 2 + b % 2) * 2 + c
            ids = first * ROWS + lax.broadcasted_iota(jnp.int32, (128, 128), 1)
            match = jnp.where(posc[rows, :] == ids, 2.0, 0.0)
            w = jnp.exp2(s - rnorm) + jnp.exp2(s - cmax[0:1, cols]) - match
            W[rows, cols] = w.astype(jnp.bfloat16)
        return carry

    lax.fori_loop(5, 8, weigh, 0)

    def query_products(first, last):
        for h in range(2):
            part = jnp.dot(W[first * 128 : last * 128], PT[h].reshape(TILE, WIDE), preferred_element_type=jnp.float32)
            GQ[first:last, :, h] = part.reshape(last - first, 2, HALF, WIDE)
        for n in range(last - 1, first - 1, -1):
            start(swap(ORDER[n]))

    def swap(k):
        n = POS[k]
        return copy(GQ.at[n, 1 - c], XQ.at[n], s_x.at[n], r_x.at[n], c=1 - c)

    def side(d):
        return xh if d == 0 else 1 - xh

    def query_sum(k, d):
        return GQ[POS[k], c, side(d)] + XQ[POS[k], side(d)]

    legs = [(4, 0, 2), (4, 1, -2), (3, 0, 1), (3, 1, 1), (5, 0, -1), (5, 1, -1),
            (2, 0, 2), (2, 1, 2), (6, 0, -2), (6, 1, -2), (1, 0, 1), (1, 1, 1), (7, 0, -1), (7, 1, -1), (0, 1, 0)]

    def leg(n):
        k, d, e = legs[n]
        where = along(2, e % NZ) if e else {}
        if n >= 6 and d:
            where["xh"] = 1 - xh
        return copy(SQ.at[n], RQ.at[n], s_gq.at[n], r_gq.at[n], **where)

    def query_send(*units):
        for k, d in units:
            n = [leg_[:2] for leg_ in legs].index((k, d))
            total = query_sum(k, d)
            for m in {(2, 0): (2, 0), (2, 1): (3,), (6, 0): (4,), (6, 1): (5, 1)}.get((k, d), ()):
                leg(m).wait_recv()
                total = total + take(RQ.at[m])
            put(SQ.at[n], total)
            start(leg(n))

    def query_swap(*ks):
        for k in ks:
            swap(k).wait_recv()

    split = (pl.ds(0, FIRST), pl.ds(FIRST, ROWS - FIRST))
    own, sp, rp, sp2, rp2 = (OWN1, OWN2), (SP1, SP2), (RP1, RP2), (SS1, SS2), (RS1, RS2)

    def plane_leg(half, e, t):
        at = (half, e - 1, t)
        return copy(sp[half].at[e - 1, t], rp[half].at[e - 1, t], s_gp.at[at], r_gp.at[at], **along(half, e))

    def plane_last(half, t):
        at = (half, 3, t)
        return copy(sp2[half].at[t - 1], rp2[half].at[t - 1], s_gp.at[at], r_gp.at[at], **along(1 - half, t))

    def passage_product(a, b):
        tx, ty = lax.rem(x + a, NX), lax.rem(y + b, NY)
        cols = pl.ds(pl.multiple_of((ty * 2 + lax.rem(tx, 2)) * 128, 128), 128)
        part = tn(W[:, cols], Q[tx // 2].reshape(TILE, WIDE))
        for half, e, t in ((0, a, b), (1, b, a)):
            rows = part[0:FIRST] if half == 0 else part[FIRST:]
            if e:
                put(sp[half].at[e - 1, t], rows)
                start(plane_leg(half, e, t))
            else:
                own[half][t] = rows

    def plane_sum(half, t):
        total = own[half][t]
        for e in (1, 3, 2):
            plane_leg(half, e, t).wait_recv()
            total = total + take(rp[half].at[e - 1, t])
        return total

    def plane_send(t):
        for half in range(2):
            put(sp2[half].at[t - 1], plane_sum(half, t))
            start(plane_last(half, t))

    query_products(5, 8)
    lax.fori_loop(0, 5, weigh, 0)
    for a, b in ((2, 2), (1, 2), (2, 1),):
        passage_product(a, b)
    query_swap(4, 3, 5)
    query_send((4, 1), (4, 0), (3, 1), (5, 1), (5, 0), (3, 0))
    for a, b in ((3, 2), (2, 3), (0, 2), (2, 0),):
        passage_product(a, b)
    query_products(0, 5)
    for a, b in ((1, 1), (3, 1), (1, 3), (3, 3),):
        passage_product(a, b)
    query_swap(2, 6, 1, 7, 0)
    query_send((1, 1), (7, 1), (0, 1), (1, 0), (7, 0))
    for a, b in ((0, 1), (1, 0), (0, 3), (3, 0), (0, 0),):
        passage_product(a, b)
    query_send((2, 1), (6, 1), (6, 0), (2, 0))
    for k in (2, 1, 3,):
        plane_send(k)
    for half in range(2):
        total = plane_sum(half, 0)
        for t in (2, 1, 3):
            plane_last(half, t).wait_recv()
            total = total + take(rp2[half].at[t - 1])
        gp_ref[split[half], :] = total * factor
    total = query_sum(0, 0)
    for n in (10, 12, 6, 8):
        leg(n).wait_recv()
        total = total + take(RQ.at[n])
    gq_ref[own_rows, :] = total * factor
    total = jnp.zeros((HALF, WIDE), jnp.float32)
    for n in (14, 11, 13, 7, 9):
        leg(n).wait_recv()
        total = total + take(RQ.at[n])
    gq_ref[other_rows, :] = total * factor
    for cp in sends:
        cp.wait_send()


def local(queries, passages, positives):
    dma = pltpu.SemaphoreType.DMA
    vmem = pl.BlockSpec(memory_space=pltpu.VMEM)
    out = pltpu.VMEM((ROWS, WIDE), jnp.float32)
    parts = (FIRST, ROWS - FIRST)
    bf16, f32, i16 = jnp.bfloat16, jnp.float32, jnp.int16
    return pl.pallas_call(
        kernel,
        out_shape=(out, out),
        in_specs=[pl.BlockSpec(memory_space=pl.ANY)] * 3,
        out_specs=(vmem, vmem),
        scratch_shapes=[
            *(pltpu.VMEM((ROWS, WIDE), bf16) for _ in range(2)),
            pltpu.VMEM((128, 128), jnp.int32),
            pltpu.VMEM((2, 8, 2, HALF, WIDE), bf16),
            pltpu.VMEM((2, 8, ROWS, WIDE), bf16),
            pltpu.VMEM((TILE, TILE), f32),
            pltpu.VMEM((TILE, TILE), bf16),
            pltpu.VMEM((TILE, 128), jnp.int32),
            pltpu.VMEM((128, 128), jnp.int32),
            pltpu.VMEM((8, TILE), f32),
            pltpu.VMEM((8, TILE), f32),
            pltpu.VMEM((16, 8, 128), f32),
            pltpu.VMEM((16, 8, 128), f32),
            pltpu.VMEM((8, 128), f32),
            pltpu.VMEM((8, 128), f32),
            pltpu.VMEM((8, 128), f32),
            pltpu.VMEM((8, 2, HALF, WIDE), f32),
            pltpu.VMEM((8, 2, 2, HALF, WIDE), f32),
            pltpu.VMEM((15, 2 * HALF + 16, 128), i16),
            pltpu.VMEM((15, 2 * HALF + 16, 128), i16),
            *(pltpu.VMEM((4, r, WIDE), f32) for r in parts),
            *(pltpu.VMEM((3, 4, 2 * r + 16, 128), i16) for _ in range(2) for r in parts),
            *(pltpu.VMEM((3, 2 * r + 16, 128), i16) for _ in range(2) for r in parts),
            dma((3,)),
            dma, dma,
            dma((2, 5, 4)), dma((2, 5, 4)),
            dma((2, 8)), dma((2, 8)),
            dma((8, 2)), dma((8, 2)),
            dma((16,)), dma((16,)),
            dma((16,)), dma((16,)),
            dma((8,)), dma((8,)),
            dma((2, 4, 4)), dma((2, 4, 4)),
            dma((15,)), dma((15,)),
        ],
        compiler_params=pltpu.CompilerParams(
            collective_id=0, has_side_effects=True, vmem_limit_bytes=60 * 1024 * 1024
        ),
    )(queries, passages, positives.reshape(128, 128))


def solution(mesh):
    split = Mesh(
        mesh.devices.reshape(NZ, NY, 2, 2, mesh.shape["rep"]),
        AXES,
    )
    return jax.shard_map(
        local,
        mesh=split,
        in_specs=(P(BATCH, "xh"), P(BATCH, "xh"), P()),
        out_specs=(P(BATCH, "xh"), P(BATCH, "xh")),
        check_vma=False,
    )
```

```python
import math

import jax
import jax.numpy as jnp
from jax import lax
from jax.experimental import pallas as pl
from jax.experimental.pallas import tpu as pltpu
from jax.sharding import Mesh
from jax.sharding import PartitionSpec as P

AXES = ("z", "y", "xl", "c", "xh")
BATCH = ("z", "y", "xl", "c")
NX, NY, NZ = 4, 4, 8
MESH = pl.DeviceIdType.MESH
ROWS = 128
HALF = 64
WIDE = 256
TILE = 1024
ORDER = (0, 1, 7, 2, 6, 3, 5, 4)
POS = tuple(ORDER.index(k) for k in range(8))
SPLIT = 4
FIRST = 64
STEP = 32000.0
LOG2E = 1.4426950408889634
LN2 = 0.6931471805599453


def put(ref, x):
    rows = x.shape[0]
    top = jnp.max(jnp.abs(x), axis=0, keepdims=True)
    power = jnp.clip(jnp.floor(jnp.log(top) * LOG2E) + 1.0, -120.0, 120.0)
    value = jnp.round(x * (STEP * jnp.exp2(-power))).astype(jnp.int32).astype(jnp.int16)
    ref[0:rows] = value[:, :128]
    ref[rows : 2 * rows] = value[:, 128:]
    both = [jnp.broadcast_to(power[:, at : at + 128], (8, 128)) for at in (0, 128)]
    ref[2 * rows :] = jnp.concatenate(both, axis=0).astype(jnp.int32).astype(jnp.int16)


def take(ref):
    rows = (ref.shape[0] - 16) // 2
    unit = jnp.exp2(ref[2 * rows :].astype(jnp.int32).astype(jnp.float32)) * (1.0 / STEP)
    value = ref[0 : 2 * rows].astype(jnp.int32).astype(jnp.float32)
    return jnp.concatenate([value[:rows] * unit[0:1], value[rows:] * unit[8:9]], axis=1)


def to_lanes(column):
    return jnp.broadcast_to(column, (128, 128)).T[:1]


def to_rows(line):
    return jnp.broadcast_to(line, (128, 128)).T


def join(stack):
    high = jnp.max(stack, axis=0)
    return high + jnp.log(jnp.sum(jnp.exp2(stack - high[None]), axis=0)) * LOG2E


def nt(a, b):
    return lax.dot_general(a, b, (((1,), (1,)), ((), ())), preferred_element_type=jnp.float32)


def tn(a, b):
    return lax.dot_general(a, b, (((0,), (0,)), ((), ())), preferred_element_type=jnp.float32)


def kernel(
    q_hbm, p_hbm, pos_hbm, gq_ref, gp_ref, q_ref, p_ref, pos_ref,
    Q, PT, S, W, posc, tmp, cmax, csum, rstat, cstat, rown, cown, rfin,
    XQ, GQ, SQ, RQ, OWN1, OWN2, SP1, SP2, RP1, RP2, SS1, SS2, RS1, RS2,
    s_in, s_xq, r_xq, s_p, r_p, s_q, r_q, s_d, r_d, s_rs, r_rs, s_cs, r_cs,
    s_x, r_x, s_gp, r_gp, s_gq, r_gq,
):
    z, y, xl, c, xh = (lax.axis_index(a) for a in AXES)
    x = xh * 2 + xl
    factor = 1.0 / math.sqrt(2 * WIDE)

    def copy(src, dst, ssem, rsem, **where):
        return pltpu.make_async_remote_copy(
            src_ref=src, dst_ref=dst, send_sem=ssem, recv_sem=rsem,
            device_id=where, device_id_type=MESH,
        )

    def plane(k):
        tx, ty = lax.rem(x + k % 4, NX), lax.rem(y + k // 4, NY)
        return tx, ty, {"xh": tx // 2, "xl": lax.rem(tx, 2), "y": ty}

    def pillar(k):
        tz, tc = lax.rem(z + k // 2, NZ), lax.rem(c + k % 2, 2)
        return tz, tc, {"z": tz, "c": tc}

    def along(axis, e):
        if axis == 0:
            t = lax.rem(x + e, NX)
            return {"xh": t // 2, "xl": lax.rem(t, 2)}
        return {"y": lax.rem(y + e, NY)} if axis == 1 else {"z": lax.rem(z + e, NZ)}

    barrier = pltpu.get_barrier_semaphore()
    near = [along(axis, e) for e in (1, 2, 3) for axis in (0, 1)]
    near += [along(2, e) for e in (1, 7, 2, 6)] + [{"c": 1 - c}]
    for where in near:
        pl.semaphore_signal(barrier, inc=1, device_id=where, device_id_type=MESH)
    loads = [
        pltpu.make_async_copy(src, dst, s_in.at[n])
        for n, (src, dst) in enumerate(((q_hbm, q_ref), (p_hbm, p_ref), (pos_hbm, pos_ref)))
    ]
    for load in loads:
        load.start()
    for load in loads:
        load.wait()
    pl.semaphore_wait(barrier, len(near))

    slot_p = y * 2 + xl
    own_rows = pl.ds(pl.multiple_of(xh * HALF, HALF), HALF)
    other_rows = pl.ds(pl.multiple_of((1 - xh) * HALF, HALF), HALF)
    sends = []

    def start(cp):
        cp.start()
        sends.append(cp)

    def plane_copy(half, phase, e, f, sender):
        first, second = (0, 1) if half == 0 else (1, 0)
        off = [0, 0]
        if phase:
            off[first] -= f
        if not sender:
            off[second if phase else first] -= e
        ox, oy = lax.rem(x + off[0] % 4, NX), lax.rem(y + off[1] % 4, NY)
        rows = pl.ds(half * HALF, HALF)
        dst = PT.at[ox // 2, oy * 2 + lax.rem(ox, 2), rows]
        src = p_ref.at[rows] if sender and f == 0 else dst
        at = (half, phase * (f + 1), e)
        return copy(src, dst, s_p.at[at], r_p.at[at], **along(second if phase else first, e))

    def ring_copy(group, hop, back, e, rows, number, sender):
        h = xh if group == 0 else 1 - xh
        src = Q.at[h, POS[-back % NZ], c, rows]
        dst = Q.at[h, POS[(-back - e) % NZ], c, rows]
        if sender and back == 0 and group == 0:
            src = q_ref.at[own_rows]
        at = (group, number)
        return copy(src, dst, s_q.at[at], r_q.at[at], **along(2, e % NZ))

    whole, low, high = pl.ds(0, HALF), pl.ds(0, 32), pl.ds(32, 32)
    hops = [(0, 0, 2, whole), (0, 0, -2, whole), (0, 0, 1, whole), (0, 0, -1, whole),
            (1, 2, 2, low), (1, -2, -2, high), (1, 2, 1, whole), (1, -2, -1, whole)]

    def ring(group, n, sender):
        return ring_copy(group, *hops[n], n, sender)

    def across(k, group, source):
        h = xh if group == 0 else 1 - xh
        src = q_ref.at[own_rows] if k == 0 and group == 0 else Q.at[h, POS[k], c]
        dst = Q.at[h, POS[k], c if source else 1 - c]
        return copy(src, dst, s_d.at[k, group], r_d.at[k, group], c=1 - c)

    def ring_take(group, n, *ks):
        for m in n:
            ring(group, m, False).wait_recv()
        for k in ks:
            start(across(k, group, True))

    start(copy(q_ref.at[other_rows], Q.at[xh, 0, c], s_xq, r_xq, **along(0, 2)))
    for e in (2, 1, 3):
        for half in range(2):
            start(plane_copy(half, 0, e, 0, True))
    for n in range(4):
        start(ring(0, n, True))
    for e in (2, 1, 3):
        for half in range(2):
            start(plane_copy(half, 1, e, 0, True))
    start(across(0, 0, True))
    Q[xh, 0, c] = q_ref[own_rows, :]
    PT[xh, slot_p] = p_ref[...]

    for s in range(16):
        line = lax.rem(z + ORDER[s // 2], NZ) * 16 + y * 4 + xl * 2 + s % 2
        tmp[...] = to_rows(pos_ref[pl.ds(line, 1), :])
        posc[s * HALF : (s + 1) * HALF] = tmp[own_rows, :]

    def plane_pass(f):
        for half in range(2):
            plane_copy(half, 0, f, 0, False).wait_recv()
            for e in (2, 1, 3):
                start(plane_copy(half, 1, e, f, True))

    copy(q_ref.at[own_rows], Q.at[1 - xh, 0, c], s_xq, r_xq, **along(0, 2)).wait_recv()
    for n in range(4):
        start(ring(1, n, True))
    start(across(0, 1, True))
    plane_pass(1)
    plane_pass(3)
    ring_take(0, (0,), 6)
    start(ring(0, 4, True))
    start(ring(0, 6, True))
    ring_take(0, (1,), 2)
    start(ring(0, 5, True))
    start(ring(0, 7, True))
    plane_pass(2)
    ring_take(0, (2,), 7)
    ring_take(0, (3,), 1)
    ring_take(1, (0,), 6)
    start(ring(1, 4, True))
    start(ring(1, 6, True))
    ring_take(1, (1,), 2)
    start(ring(1, 5, True))
    start(ring(1, 7, True))
    ring_take(1, (2,), 7)
    ring_take(1, (3,), 1)
    for half in range(2):
        for f in range(4):
            for e in (1, 2, 3):
                plane_copy(half, 1, e, f, False).wait_recv()
    ring_take(0, (6,), 5)
    ring_take(0, (7,), 3)
    ring_take(0, (4, 5), 4)

    def tile_z(n):
        odd = lax.rem(n, 2) == 1
        k = jnp.where(odd, (n + 1) // 2, NZ - n // 2)
        return lax.rem(z + k, NZ)

    def score_dots(first, last):
        for n in range(first, last):
            for group in range(2):
                across(ORDER[n], group, False).wait_recv()
        part = [
            nt(Q[h, first:last].reshape((last - first) * 128, WIDE), PT[h].reshape(TILE, WIDE))
            for h in range(2)
        ]
        S[first * 128 : last * 128] = (part[0] + part[1]) * (factor * LOG2E)

    def score(n, carry):
        s = S[pl.ds(pl.multiple_of(n * 128, 128), 128)]
        high = jnp.max(s, axis=1, keepdims=True)
        total = jnp.sum(jnp.exp2(s - high), axis=1, keepdims=True)
        rown[pl.ds(tile_z(n), 1)] = to_lanes(high + jnp.log(total) * LOG2E)
        chigh = jnp.max(s, axis=0, keepdims=True)
        cmax[pl.ds(n, 1)] = chigh
        csum[pl.ds(n, 1)] = jnp.sum(jnp.exp2(s - chigh), axis=0, keepdims=True)
        return carry

    score_dots(0, SPLIT)
    lax.fori_loop(0, SPLIT, score, 0)
    ring_take(1, (6,), 5)
    ring_take(1, (7,), 3)
    ring_take(1, (4, 5), 4)
    score_dots(SPLIT, 8)
    lax.fori_loop(SPLIT, 8, score, 0)
    for k in sorted(range(1, 16), key=lambda k: -min(k // 2, 8 - k // 2)):
        start(copy(rown, rstat.at[k], s_rs.at[k], r_rs.at[k], **pillar(k)[2]))
    chigh = jnp.max(cmax[...], axis=0, keepdims=True)
    ctotal = jnp.sum(csum[...] * jnp.exp2(cmax[...] - chigh), axis=0, keepdims=True)
    cnorm = chigh + jnp.log(ctotal) * LOG2E
    for b in range(8):
        cown[b : b + 1] = cnorm[:, b * 128 : (b + 1) * 128]
    rstat[0] = rown[...]
    cstat[0] = cown[...]
    for k in sorted(range(1, 16), key=lambda k: -min(k % 4, -k % 4) - min(k // 4, 4 - k // 4)):
        start(copy(cown, cstat.at[k], s_cs.at[k], r_cs.at[k], **plane(k)[2]))
    for k in range(1, 16):
        copy(rown, rstat.at[k], s_rs.at[k], r_rs.at[k], **pillar(k)[2]).wait_recv()
        copy(cown, cstat.at[k], s_cs.at[k], r_cs.at[k], **plane(k)[2]).wait_recv()
    rown2 = join(rstat[...])
    cown2 = join(cstat[...])
    cmax[0:1] = jnp.concatenate([cown2[b : b + 1] for b in range(8)], axis=1)
    rfin[...] = rown2

    def weigh(i, carry):
        rows = pl.ds(pl.multiple_of(i * 128, 128), 128)
        rnorm = to_rows(rfin[pl.ds(tile_z(i), 1), :])
        for b in range(8):
            cols = slice(b * 128, (b + 1) * 128)
            s = S[rows, cols]
            first = ((z * 4 + b // 2) * 2 + b % 2) * 2 + c
            ids = first * ROWS + lax.broadcasted_iota(jnp.int32, (128, 128), 1)
            match = jnp.where(posc[rows, :] == ids, 2.0, 0.0)
            w = jnp.exp2(s - rnorm) + jnp.exp2(s - cmax[0:1, cols]) - match
            W[rows, cols] = w.astype(jnp.bfloat16)
        return carry

    lax.fori_loop(5, 8, weigh, 0)

    def query_products(first, last):
        for h in range(2):
            part = jnp.dot(W[first * 128 : last * 128], PT[h].reshape(TILE, WIDE), preferred_element_type=jnp.float32)
            GQ[first:last, :, h] = part.reshape(last - first, 2, HALF, WIDE)
        for n in range(last - 1, first - 1, -1):
            start(swap(ORDER[n]))

    def swap(k):
        n = POS[k]
        return copy(GQ.at[n, 1 - c], XQ.at[n], s_x.at[n], r_x.at[n], c=1 - c)

    def side(d):
        return xh if d == 0 else 1 - xh

    def query_sum(k, d):
        return GQ[POS[k], c, side(d)] + XQ[POS[k], side(d)]

    legs = [(4, 0, 2), (4, 1, -2), (3, 0, 1), (3, 1, 1), (5, 0, -1), (5, 1, -1),
            (2, 0, 2), (2, 1, 2), (6, 0, -2), (6, 1, -2), (1, 0, 1), (1, 1, 1), (7, 0, -1), (7, 1, -1), (0, 1, 0)]

    def leg(n):
        k, d, e = legs[n]
        where = along(2, e % NZ) if e else {}
        if n >= 6 and d:
            where["xh"] = 1 - xh
        return copy(SQ.at[n], RQ.at[n], s_gq.at[n], r_gq.at[n], **where)

    def query_send(*units):
        for k, d in units:
            n = [leg_[:2] for leg_ in legs].index((k, d))
            total = query_sum(k, d)
            for m in {(2, 0): (2, 0), (2, 1): (3,), (6, 0): (4,), (6, 1): (5, 1)}.get((k, d), ()):
                leg(m).wait_recv()
                total = total + take(RQ.at[m])
            put(SQ.at[n], total)
            start(leg(n))

    def query_swap(*ks):
        for k in ks:
            swap(k).wait_recv()

    split = (pl.ds(0, FIRST), pl.ds(FIRST, ROWS - FIRST))
    own, sp, rp, sp2, rp2 = (OWN1, OWN2), (SP1, SP2), (RP1, RP2), (SS1, SS2), (RS1, RS2)

    def plane_leg(half, e, t):
        at = (half, e - 1, t)
        return copy(sp[half].at[e - 1, t], rp[half].at[e - 1, t], s_gp.at[at], r_gp.at[at], **along(half, e))

    def plane_last(half, t):
        at = (half, 3, t)
        return copy(sp2[half].at[t - 1], rp2[half].at[t - 1], s_gp.at[at], r_gp.at[at], **along(1 - half, t))

    def passage_product(a, b):
        tx, ty = lax.rem(x + a, NX), lax.rem(y + b, NY)
        cols = pl.ds(pl.multiple_of((ty * 2 + lax.rem(tx, 2)) * 128, 128), 128)
        part = tn(W[:, cols], Q[tx // 2].reshape(TILE, WIDE))
        for half, e, t in ((0, a, b), (1, b, a)):
            rows = part[0:FIRST] if half == 0 else part[FIRST:]
            if e:
                put(sp[half].at[e - 1, t], rows)
                start(plane_leg(half, e, t))
            else:
                own[half][t] = rows

    def plane_sum(half, t):
        total = own[half][t]
        for e in (1, 3, 2):
            plane_leg(half, e, t).wait_recv()
            total = total + take(rp[half].at[e - 1, t])
        return total

    def plane_send(t):
        for half in range(2):
            put(sp2[half].at[t - 1], plane_sum(half, t))
            start(plane_last(half, t))

    query_products(5, 8)
    lax.fori_loop(0, 5, weigh, 0)
    for a, b in ((2, 2), (1, 2), (2, 1),):
        passage_product(a, b)
    query_swap(4, 3, 5)
    query_send((4, 1), (4, 0), (3, 1), (5, 1), (5, 0), (3, 0))
    for a, b in ((3, 2), (2, 3), (0, 2), (2, 0),):
        passage_product(a, b)
    query_products(0, 5)
    for a, b in ((1, 1), (3, 1), (1, 3), (3, 3),):
        passage_product(a, b)
    for a, b in ((0, 1), (1, 0), (0, 3), (3, 0), (0, 0),):
        passage_product(a, b)
    query_swap(2, 6, 1, 7, 0)
    for k in (2,):
        plane_send(k)
    query_send((2, 1), (6, 1))
    query_send((6, 0), (2, 0))
    for k in (1, 3,):
        plane_send(k)
    query_send((1, 1), (7, 1), (0, 1), (1, 0), (7, 0))
    totals = [plane_sum(half, 0) for half in range(2)]
    for half in range(2):
        total = totals[half]
        for t in (2, 1, 3):
            plane_last(half, t).wait_recv()
            total = total + take(rp2[half].at[t - 1])
        gp_ref[split[half], :] = total * factor
    total = query_sum(0, 0)
    for n in (10, 12, 6, 8):
        leg(n).wait_recv()
        total = total + take(RQ.at[n])
    gq_ref[own_rows, :] = total * factor
    total = jnp.zeros((HALF, WIDE), jnp.float32)
    for n in (14, 11, 13, 7, 9):
        leg(n).wait_recv()
        total = total + take(RQ.at[n])
    gq_ref[other_rows, :] = total * factor
    for cp in sends:
        cp.wait_send()


def local(queries, passages, positives):
    dma = pltpu.SemaphoreType.DMA
    vmem = pl.BlockSpec(memory_space=pltpu.VMEM)
    out = pltpu.VMEM((ROWS, WIDE), jnp.float32)
    parts = (FIRST, ROWS - FIRST)
    bf16, f32, i16 = jnp.bfloat16, jnp.float32, jnp.int16
    return pl.pallas_call(
        kernel,
        out_shape=(out, out),
        in_specs=[pl.BlockSpec(memory_space=pl.ANY)] * 3,
        out_specs=(vmem, vmem),
        scratch_shapes=[
            *(pltpu.VMEM((ROWS, WIDE), bf16) for _ in range(2)),
            pltpu.VMEM((128, 128), jnp.int32),
            pltpu.VMEM((2, 8, 2, HALF, WIDE), bf16),
            pltpu.VMEM((2, 8, ROWS, WIDE), bf16),
            pltpu.VMEM((TILE, TILE), f32),
            pltpu.VMEM((TILE, TILE), bf16),
            pltpu.VMEM((TILE, 128), jnp.int32),
            pltpu.VMEM((128, 128), jnp.int32),
            pltpu.VMEM((8, TILE), f32),
            pltpu.VMEM((8, TILE), f32),
            pltpu.VMEM((16, 8, 128), f32),
            pltpu.VMEM((16, 8, 128), f32),
            pltpu.VMEM((8, 128), f32),
            pltpu.VMEM((8, 128), f32),
            pltpu.VMEM((8, 128), f32),
            pltpu.VMEM((8, 2, HALF, WIDE), f32),
            pltpu.VMEM((8, 2, 2, HALF, WIDE), f32),
            pltpu.VMEM((15, 2 * HALF + 16, 128), i16),
            pltpu.VMEM((15, 2 * HALF + 16, 128), i16),
            *(pltpu.VMEM((4, r, WIDE), f32) for r in parts),
            *(pltpu.VMEM((3, 4, 2 * r + 16, 128), i16) for _ in range(2) for r in parts),
            *(pltpu.VMEM((3, 2 * r + 16, 128), i16) for _ in range(2) for r in parts),
            dma((3,)),
            dma, dma,
            dma((2, 5, 4)), dma((2, 5, 4)),
            dma((2, 8)), dma((2, 8)),
            dma((8, 2)), dma((8, 2)),
            dma((16,)), dma((16,)),
            dma((16,)), dma((16,)),
            dma((8,)), dma((8,)),
            dma((2, 4, 4)), dma((2, 4, 4)),
            dma((15,)), dma((15,)),
        ],
        compiler_params=pltpu.CompilerParams(
            collective_id=0, has_side_effects=True, vmem_limit_bytes=60 * 1024 * 1024
        ),
    )(queries, passages, positives.reshape(128, 128))


def solution(mesh):
    split = Mesh(
        mesh.devices.reshape(NZ, NY, 2, 2, mesh.shape["rep"]),
        AXES,
    )
    return jax.shard_map(
        local,
        mesh=split,
        in_specs=(P(BATCH, "xh"), P(BATCH, "xh"), P()),
        out_specs=(P(BATCH, "xh"), P(BATCH, "xh")),
        check_vma=False,
    )
```

```python
import math

import jax
import jax.numpy as jnp
from jax import lax
from jax.experimental import pallas as pl
from jax.experimental.pallas import tpu as pltpu
from jax.sharding import Mesh
from jax.sharding import PartitionSpec as P

AXES = ("z", "y", "xl", "c", "xh")
BATCH = ("z", "y", "xl", "c")
NX, NY, NZ = 4, 4, 8
MESH = pl.DeviceIdType.MESH
ROWS = 128
HALF = 64
WIDE = 256
TILE = 1024
ORDER = (0, 1, 7, 2, 6, 3, 5, 4)
POS = tuple(ORDER.index(k) for k in range(8))
SPLIT = 4
FIRST = 64
STEP = 32000.0
LOG2E = 1.4426950408889634
LN2 = 0.6931471805599453


def put(ref, x):
    rows = x.shape[0]
    top = jnp.max(jnp.abs(x), axis=0, keepdims=True)
    power = jnp.clip(jnp.floor(jnp.log(top) * LOG2E) + 1.0, -120.0, 120.0)
    value = jnp.round(x * (STEP * jnp.exp2(-power))).astype(jnp.int32).astype(jnp.int16)
    ref[0:rows] = value[:, :128]
    ref[rows : 2 * rows] = value[:, 128:]
    both = [jnp.broadcast_to(power[:, at : at + 128], (8, 128)) for at in (0, 128)]
    ref[2 * rows :] = jnp.concatenate(both, axis=0).astype(jnp.int32).astype(jnp.int16)


def take(ref):
    rows = (ref.shape[0] - 16) // 2
    unit = jnp.exp2(ref[2 * rows :].astype(jnp.int32).astype(jnp.float32)) * (1.0 / STEP)
    value = ref[0 : 2 * rows].astype(jnp.int32).astype(jnp.float32)
    return jnp.concatenate([value[:rows] * unit[0:1], value[rows:] * unit[8:9]], axis=1)


def to_lanes(column):
    return jnp.broadcast_to(column, (128, 128)).T[:1]


def to_rows(line):
    return jnp.broadcast_to(line, (128, 128)).T


def join(stack):
    high = jnp.max(stack, axis=0)
    return high + jnp.log(jnp.sum(jnp.exp2(stack - high[None]), axis=0)) * LOG2E


def nt(a, b):
    return lax.dot_general(a, b, (((1,), (1,)), ((), ())), preferred_element_type=jnp.float32)


def tn(a, b):
    return lax.dot_general(a, b, (((0,), (0,)), ((), ())), preferred_element_type=jnp.float32)


def kernel(
    q_hbm, p_hbm, pos_hbm, gq_ref, gp_ref, q_ref, p_ref, pos_ref,
    Q, PT, S, W, posc, tmp, cmax, csum, rstat, cstat, rown, cown, rfin,
    XQ, GQ, SQ, RQ, OWN1, OWN2, SP1, SP2, RP1, RP2, SS1, SS2, RS1, RS2,
    s_in, s_xq, r_xq, s_p, r_p, s_q, r_q, s_d, r_d, s_rs, r_rs, s_cs, r_cs,
    s_x, r_x, s_gp, r_gp, s_gq, r_gq,
):
    z, y, xl, c, xh = (lax.axis_index(a) for a in AXES)
    x = xh * 2 + xl
    factor = 1.0 / math.sqrt(2 * WIDE)

    def copy(src, dst, ssem, rsem, **where):
        return pltpu.make_async_remote_copy(
            src_ref=src, dst_ref=dst, send_sem=ssem, recv_sem=rsem,
            device_id=where, device_id_type=MESH,
        )

    def plane(k):
        tx, ty = lax.rem(x + k % 4, NX), lax.rem(y + k // 4, NY)
        return tx, ty, {"xh": tx // 2, "xl": lax.rem(tx, 2), "y": ty}

    def pillar(k):
        tz, tc = lax.rem(z + k // 2, NZ), lax.rem(c + k % 2, 2)
        return tz, tc, {"z": tz, "c": tc}

    def along(axis, e):
        if axis == 0:
            t = lax.rem(x + e, NX)
            return {"xh": t // 2, "xl": lax.rem(t, 2)}
        return {"y": lax.rem(y + e, NY)} if axis == 1 else {"z": lax.rem(z + e, NZ)}

    barrier = pltpu.get_barrier_semaphore()
    near = [along(axis, e) for e in (1, 2, 3) for axis in (0, 1)]
    near += [along(2, e) for e in (1, 7, 2, 6)] + [{"c": 1 - c}]
    for where in near:
        pl.semaphore_signal(barrier, inc=1, device_id=where, device_id_type=MESH)
    loads = [
        pltpu.make_async_copy(src, dst, s_in.at[n])
        for n, (src, dst) in enumerate(((q_hbm, q_ref), (p_hbm, p_ref), (pos_hbm, pos_ref)))
    ]
    for load in loads:
        load.start()
    for load in loads:
        load.wait()
    pl.semaphore_wait(barrier, len(near))

    slot_p = y * 2 + xl
    own_rows = pl.ds(pl.multiple_of(xh * HALF, HALF), HALF)
    other_rows = pl.ds(pl.multiple_of((1 - xh) * HALF, HALF), HALF)
    sends = []

    def start(cp):
        cp.start()
        sends.append(cp)

    def plane_copy(half, phase, e, f, sender):
        first, second = (0, 1) if half == 0 else (1, 0)
        off = [0, 0]
        if phase:
            off[first] -= f
        if not sender:
            off[second if phase else first] -= e
        ox, oy = lax.rem(x + off[0] % 4, NX), lax.rem(y + off[1] % 4, NY)
        rows = pl.ds(half * HALF, HALF)
        dst = PT.at[ox // 2, oy * 2 + lax.rem(ox, 2), rows]
        src = p_ref.at[rows] if sender and f == 0 else dst
        at = (half, phase * (f + 1), e)
        return copy(src, dst, s_p.at[at], r_p.at[at], **along(second if phase else first, e))

    def ring_copy(group, hop, back, e, rows, number, sender):
        h = xh if group == 0 else 1 - xh
        src = Q.at[h, POS[-back % NZ], c, rows]
        dst = Q.at[h, POS[(-back - e) % NZ], c, rows]
        if sender and back == 0 and group == 0:
            src = q_ref.at[own_rows]
        at = (group, number)
        return copy(src, dst, s_q.at[at], r_q.at[at], **along(2, e % NZ))

    whole, low, high = pl.ds(0, HALF), pl.ds(0, 32), pl.ds(32, 32)
    hops = [(0, 0, 2, whole), (0, 0, -2, whole), (0, 0, 1, whole), (0, 0, -1, whole),
            (1, 2, 2, low), (1, -2, -2, high), (1, 2, 1, whole), (1, -2, -1, whole)]

    def ring(group, n, sender):
        return ring_copy(group, *hops[n], n, sender)

    def across(k, group, source):
        h = xh if group == 0 else 1 - xh
        src = q_ref.at[own_rows] if k == 0 and group == 0 else Q.at[h, POS[k], c]
        dst = Q.at[h, POS[k], c if source else 1 - c]
        return copy(src, dst, s_d.at[k, group], r_d.at[k, group], c=1 - c)

    def ring_take(group, n, *ks):
        for m in n:
            ring(group, m, False).wait_recv()
        for k in ks:
            start(across(k, group, True))

    start(copy(q_ref.at[other_rows], Q.at[xh, 0, c], s_xq, r_xq, **along(0, 2)))
    for e in (2, 1, 3):
        for half in range(2):
            start(plane_copy(half, 0, e, 0, True))
    for n in range(4):
        start(ring(0, n, True))
    for e in (2, 1, 3):
        for half in range(2):
            start(plane_copy(half, 1, e, 0, True))
    start(across(0, 0, True))
    Q[xh, 0, c] = q_ref[own_rows, :]
    PT[xh, slot_p] = p_ref[...]

    for s in range(16):
        line = lax.rem(z + ORDER[s // 2], NZ) * 16 + y * 4 + xl * 2 + s % 2
        tmp[...] = to_rows(pos_ref[pl.ds(line, 1), :])
        posc[s * HALF : (s + 1) * HALF] = tmp[own_rows, :]

    def plane_pass(f):
        for half in range(2):
            plane_copy(half, 0, f, 0, False).wait_recv()
            for e in (2, 1, 3):
                start(plane_copy(half, 1, e, f, True))

    copy(q_ref.at[own_rows], Q.at[1 - xh, 0, c], s_xq, r_xq, **along(0, 2)).wait_recv()
    for n in range(4):
        start(ring(1, n, True))
    start(across(0, 1, True))
    plane_pass(1)
    plane_pass(3)
    ring_take(0, (0,), 6)
    start(ring(0, 4, True))
    start(ring(0, 6, True))
    ring_take(0, (1,), 2)
    start(ring(0, 5, True))
    start(ring(0, 7, True))
    plane_pass(2)
    ring_take(0, (2,), 7)
    ring_take(0, (3,), 1)
    ring_take(1, (0,), 6)
    start(ring(1, 4, True))
    start(ring(1, 6, True))
    ring_take(1, (1,), 2)
    start(ring(1, 5, True))
    start(ring(1, 7, True))
    ring_take(1, (2,), 7)
    ring_take(1, (3,), 1)
    for half in range(2):
        for f in range(4):
            for e in (1, 2, 3):
                plane_copy(half, 1, e, f, False).wait_recv()
    ring_take(0, (6,), 5)
    ring_take(0, (7,), 3)
    ring_take(0, (4, 5), 4)

    def tile_z(n):
        odd = lax.rem(n, 2) == 1
        k = jnp.where(odd, (n + 1) // 2, NZ - n // 2)
        return lax.rem(z + k, NZ)

    def score_dots(first, last):
        for n in range(first, last):
            for group in range(2):
                across(ORDER[n], group, False).wait_recv()
        part = [
            nt(Q[h, first:last].reshape((last - first) * 128, WIDE), PT[h].reshape(TILE, WIDE))
            for h in range(2)
        ]
        S[first * 128 : last * 128] = (part[0] + part[1]) * (factor * LOG2E)

    def score(n, carry):
        s = S[pl.ds(pl.multiple_of(n * 128, 128), 128)]
        high = jnp.max(s, axis=1, keepdims=True)
        total = jnp.sum(jnp.exp2(s - high), axis=1, keepdims=True)
        rown[pl.ds(tile_z(n), 1)] = to_lanes(high + jnp.log(total) * LOG2E)
        chigh = jnp.max(s, axis=0, keepdims=True)
        cmax[pl.ds(n, 1)] = chigh
        csum[pl.ds(n, 1)] = jnp.sum(jnp.exp2(s - chigh), axis=0, keepdims=True)
        return carry

    score_dots(0, SPLIT)
    lax.fori_loop(0, SPLIT, score, 0, unroll=2)
    ring_take(1, (6,), 5)
    ring_take(1, (7,), 3)
    ring_take(1, (4, 5), 4)
    score_dots(SPLIT, 8)
    lax.fori_loop(SPLIT, 8, score, 0, unroll=2)
    for k in sorted(range(1, 16), key=lambda k: -min(k // 2, 8 - k // 2)):
        start(copy(rown, rstat.at[k], s_rs.at[k], r_rs.at[k], **pillar(k)[2]))
    chigh = jnp.max(cmax[...], axis=0, keepdims=True)
    ctotal = jnp.sum(csum[...] * jnp.exp2(cmax[...] - chigh), axis=0, keepdims=True)
    cnorm = chigh + jnp.log(ctotal) * LOG2E
    for b in range(8):
        cown[b : b + 1] = cnorm[:, b * 128 : (b + 1) * 128]
    rstat[0] = rown[...]
    cstat[0] = cown[...]
    for k in sorted(range(1, 16), key=lambda k: -min(k % 4, -k % 4) - min(k // 4, 4 - k // 4)):
        start(copy(cown, cstat.at[k], s_cs.at[k], r_cs.at[k], **plane(k)[2]))
    for k in range(1, 16):
        copy(rown, rstat.at[k], s_rs.at[k], r_rs.at[k], **pillar(k)[2]).wait_recv()
        copy(cown, cstat.at[k], s_cs.at[k], r_cs.at[k], **plane(k)[2]).wait_recv()
    rown2 = join(rstat[...])
    cown2 = join(cstat[...])
    cmax[0:1] = jnp.concatenate([cown2[b : b + 1] for b in range(8)], axis=1)
    rfin[...] = rown2

    def weigh(i, carry):
        rows = pl.ds(pl.multiple_of(i * 128, 128), 128)
        rnorm = to_rows(rfin[pl.ds(tile_z(i), 1), :])
        for b in range(8):
            cols = slice(b * 128, (b + 1) * 128)
            s = S[rows, cols]
            first = ((z * 4 + b // 2) * 2 + b % 2) * 2 + c
            ids = first * ROWS + lax.broadcasted_iota(jnp.int32, (128, 128), 1)
            match = jnp.where(posc[rows, :] == ids, 2.0, 0.0)
            w = jnp.exp2(s - rnorm) + jnp.exp2(s - cmax[0:1, cols]) - match
            W[rows, cols] = w.astype(jnp.bfloat16)
        return carry

    lax.fori_loop(5, 8, weigh, 0)

    def query_products(first, last):
        for h in range(2):
            part = jnp.dot(W[first * 128 : last * 128], PT[h].reshape(TILE, WIDE), preferred_element_type=jnp.float32)
            GQ[first:last, :, h] = part.reshape(last - first, 2, HALF, WIDE)
        for n in range(last - 1, first - 1, -1):
            start(swap(ORDER[n]))

    def swap(k):
        n = POS[k]
        return copy(GQ.at[n, 1 - c], XQ.at[n], s_x.at[n], r_x.at[n], c=1 - c)

    def side(d):
        return xh if d == 0 else 1 - xh

    def query_sum(k, d):
        return GQ[POS[k], c, side(d)] + XQ[POS[k], side(d)]

    legs = [(4, 0, 2), (4, 1, -2), (3, 0, 1), (3, 1, 1), (5, 0, -1), (5, 1, -1),
            (2, 0, 2), (2, 1, 2), (6, 0, -2), (6, 1, -2), (1, 0, 1), (1, 1, 1), (7, 0, -1), (7, 1, -1), (0, 1, 0)]

    def leg(n):
        k, d, e = legs[n]
        where = along(2, e % NZ) if e else {}
        if n >= 6 and d:
            where["xh"] = 1 - xh
        return copy(SQ.at[n], RQ.at[n], s_gq.at[n], r_gq.at[n], **where)

    def query_send(*units):
        for k, d in units:
            n = [leg_[:2] for leg_ in legs].index((k, d))
            total = query_sum(k, d)
            for m in {(2, 0): (2, 0), (2, 1): (3,), (6, 0): (4,), (6, 1): (5, 1)}.get((k, d), ()):
                leg(m).wait_recv()
                total = total + take(RQ.at[m])
            put(SQ.at[n], total)
            start(leg(n))

    def query_swap(*ks):
        for k in ks:
            swap(k).wait_recv()

    split = (pl.ds(0, FIRST), pl.ds(FIRST, ROWS - FIRST))
    own, sp, rp, sp2, rp2 = (OWN1, OWN2), (SP1, SP2), (RP1, RP2), (SS1, SS2), (RS1, RS2)

    def plane_leg(half, e, t):
        at = (half, e - 1, t)
        return copy(sp[half].at[e - 1, t], rp[half].at[e - 1, t], s_gp.at[at], r_gp.at[at], **along(half, e))

    def plane_last(half, t):
        at = (half, 3, t)
        return copy(sp2[half].at[t - 1], rp2[half].at[t - 1], s_gp.at[at], r_gp.at[at], **along(1 - half, t))

    def passage_product(a, b):
        tx, ty = lax.rem(x + a, NX), lax.rem(y + b, NY)
        cols = pl.ds(pl.multiple_of((ty * 2 + lax.rem(tx, 2)) * 128, 128), 128)
        part = tn(W[:, cols], Q[tx // 2].reshape(TILE, WIDE))
        for half, e, t in ((0, a, b), (1, b, a)):
            rows = part[0:FIRST] if half == 0 else part[FIRST:]
            if e:
                put(sp[half].at[e - 1, t], rows)
                start(plane_leg(half, e, t))
            else:
                own[half][t] = rows

    def plane_sum(half, t):
        total = own[half][t]
        for e in (1, 3, 2):
            plane_leg(half, e, t).wait_recv()
            total = total + take(rp[half].at[e - 1, t])
        return total

    def plane_send(t):
        for half in range(2):
            put(sp2[half].at[t - 1], plane_sum(half, t))
            start(plane_last(half, t))

    query_products(5, 8)
    lax.fori_loop(0, 5, weigh, 0)
    for a, b in ((2, 2), (1, 2), (2, 1),):
        passage_product(a, b)
    query_swap(4, 3, 5)
    query_send((4, 1), (4, 0), (3, 1), (5, 1), (5, 0), (3, 0))
    for a, b in ((3, 2), (2, 3), (0, 2), (2, 0),):
        passage_product(a, b)
    query_products(0, 5)
    for a, b in ((1, 1), (3, 1), (1, 3), (3, 3),):
        passage_product(a, b)
    for a, b in ((0, 1), (1, 0), (0, 3), (3, 0), (0, 0),):
        passage_product(a, b)
    query_swap(2, 6, 1, 7, 0)
    for k in (2,):
        plane_send(k)
    query_send((2, 1), (6, 1))
    query_send((6, 0), (2, 0))
    for k in (1, 3,):
        plane_send(k)
    query_send((1, 1), (7, 1), (0, 1), (1, 0), (7, 0))
    totals = [plane_sum(half, 0) for half in range(2)]
    for half in range(2):
        total = totals[half]
        for t in (2, 1, 3):
            plane_last(half, t).wait_recv()
            total = total + take(rp2[half].at[t - 1])
        gp_ref[split[half], :] = total * factor
    total = query_sum(0, 0)
    for n in (10, 12, 6, 8):
        leg(n).wait_recv()
        total = total + take(RQ.at[n])
    gq_ref[own_rows, :] = total * factor
    total = jnp.zeros((HALF, WIDE), jnp.float32)
    for n in (14, 11, 13, 7, 9):
        leg(n).wait_recv()
        total = total + take(RQ.at[n])
    gq_ref[other_rows, :] = total * factor
    for cp in sends:
        cp.wait_send()


def local(queries, passages, positives):
    dma = pltpu.SemaphoreType.DMA
    vmem = pl.BlockSpec(memory_space=pltpu.VMEM)
    out = pltpu.VMEM((ROWS, WIDE), jnp.float32)
    parts = (FIRST, ROWS - FIRST)
    bf16, f32, i16 = jnp.bfloat16, jnp.float32, jnp.int16
    return pl.pallas_call(
        kernel,
        out_shape=(out, out),
        in_specs=[pl.BlockSpec(memory_space=pl.ANY)] * 3,
        out_specs=(vmem, vmem),
        scratch_shapes=[
            *(pltpu.VMEM((ROWS, WIDE), bf16) for _ in range(2)),
            pltpu.VMEM((128, 128), jnp.int32),
            pltpu.VMEM((2, 8, 2, HALF, WIDE), bf16),
            pltpu.VMEM((2, 8, ROWS, WIDE), bf16),
            pltpu.VMEM((TILE, TILE), f32),
            pltpu.VMEM((TILE, TILE), bf16),
            pltpu.VMEM((TILE, 128), jnp.int32),
            pltpu.VMEM((128, 128), jnp.int32),
            pltpu.VMEM((8, TILE), f32),
            pltpu.VMEM((8, TILE), f32),
            pltpu.VMEM((16, 8, 128), f32),
            pltpu.VMEM((16, 8, 128), f32),
            pltpu.VMEM((8, 128), f32),
            pltpu.VMEM((8, 128), f32),
            pltpu.VMEM((8, 128), f32),
            pltpu.VMEM((8, 2, HALF, WIDE), f32),
            pltpu.VMEM((8, 2, 2, HALF, WIDE), f32),
            pltpu.VMEM((15, 2 * HALF + 16, 128), i16),
            pltpu.VMEM((15, 2 * HALF + 16, 128), i16),
            *(pltpu.VMEM((4, r, WIDE), f32) for r in parts),
            *(pltpu.VMEM((3, 4, 2 * r + 16, 128), i16) for _ in range(2) for r in parts),
            *(pltpu.VMEM((3, 2 * r + 16, 128), i16) for _ in range(2) for r in parts),
            dma((3,)),
            dma, dma,
            dma((2, 5, 4)), dma((2, 5, 4)),
            dma((2, 8)), dma((2, 8)),
            dma((8, 2)), dma((8, 2)),
            dma((16,)), dma((16,)),
            dma((16,)), dma((16,)),
            dma((8,)), dma((8,)),
            dma((2, 4, 4)), dma((2, 4, 4)),
            dma((15,)), dma((15,)),
        ],
        compiler_params=pltpu.CompilerParams(
            collective_id=0, has_side_effects=True, vmem_limit_bytes=60 * 1024 * 1024
        ),
    )(queries, passages, positives.reshape(128, 128))


def solution(mesh):
    split = Mesh(
        mesh.devices.reshape(NZ, NY, 2, 2, mesh.shape["rep"]),
        AXES,
    )
    return jax.shard_map(
        local,
        mesh=split,
        in_specs=(P(BATCH, "xh"), P(BATCH, "xh"), P()),
        out_specs=(P(BATCH, "xh"), P(BATCH, "xh")),
        check_vma=False,
    )
```
